32 devices in a mesh: section: 4 (over y, core), replica: 8 (over z, x).
Axes of the slice: x: 2, y: 2, z: 4, core: 2. Of those that a mesh axis runs over, the one named last changes fastest.
Arguments:
- gradient: bfloat16 [512, 32768], P('section', 'replica'), may hold values from -1300 to 1300
- residual: float32 [512, 32768], P('section', 'replica'), may hold values from -6 to 6
- block_ids: int32 [4, 64], P('section', 'replica'), may hold values from 0 to 15, as said below
- block_counts: int32 [4, 8], P('section', 'replica'), may hold values from 1 to 8, as said below
Outputs:
- new_residual: float32 [512, 32768], P('section', 'replica')
- update: bfloat16 [512, 4096], P('section', 'replica')
The draws below stay inside these ranges and needn't reach their ends.
Inputs may be any that keep to these rules, and one draw needn't show every extreme that they name: `block_ids`: each device's 8 block numbers are distinct; only the first block_counts of them are selected. `block_counts`: in every section some replica selects exactly 8 blocks; the others select at most 4.
All inputs are finite; a program needn't handle non-finite values.
Results may differ from the reference program's by a relative error of at most 0.013.
Values may be sent and summed in bfloat16 or wider, within the bound.
A program may use at most 64 MiB of HBM per device.

```python
import math
import jax
import jax.numpy as jnp
from jax import lax

D = 4096
ROWS = 128
BLK = 8
KMAX = 8
SECTIONS = 4
REPLICAS = 8


def draw_gradient(key, part):
    key_rows, key_base, key_common, key_level, key_mix, key_slice, key_column = jax.random.split(key, 7)
    slice_width = D // REPLICAS
    row_scale = jnp.exp(jax.random.uniform(key_rows, (SECTIONS * ROWS, REPLICAS, 1), jnp.float32, 0.0, math.log(10.0)))
    section_of_row = (jnp.arange(SECTIONS * ROWS, dtype=jnp.int32) // ROWS).astype(jnp.int32)
    section_scale = 1.0 + 2.0 * section_of_row.astype(jnp.float32) / max(SECTIONS - 1, 1)
    slice_of_column = (jnp.arange(D, dtype=jnp.int32) // slice_width).astype(jnp.int32)
    slice_scale = jnp.exp(jax.random.uniform(key_slice, (REPLICAS,), jnp.float32, 0.0, math.log(4.0)))
    column_rough = jax.random.uniform(key_column, (D,), jnp.float32, 0.6, 1.4)
    column_scale = slice_scale[slice_of_column] * column_rough
    section_level = jax.random.uniform(key_level, (SECTIONS,), jnp.float32, 0.0, 1.2)
    slice_mix = jax.random.uniform(key_mix, (SECTIONS, REPLICAS), jnp.float32, 0.0, 1.0)
    mix_weight = section_level[:, None] * slice_mix
    weight_grid = mix_weight[section_of_row][:, slice_of_column]
    base_draw = jnp.clip(jax.random.normal(key_base, (SECTIONS * ROWS, REPLICAS, D), jnp.float32), -4.0, 4.0)
    common_part = jnp.clip(jax.random.normal(key_common, (SECTIONS * ROWS, 1, D), jnp.float32), -3.0, 3.0)
    base_draw = base_draw + weight_grid[:, None, :] * common_part
    values = base_draw * row_scale * section_scale[:, None, None] * column_scale[None, None, :]
    return values.reshape(SECTIONS * ROWS, REPLICAS * D).astype(jnp.bfloat16)


def draw_block_ids(key, part):
    block_total = ROWS // BLK
    scores = jax.random.randint(key, (SECTIONS, REPLICAS, block_total), 0, 1 << 20) * block_total + jnp.arange(block_total, dtype=jnp.int32)
    ordering = jnp.argsort(scores, axis=-1, stable=True)
    return ordering[..., :KMAX].reshape(SECTIONS, REPLICAS * KMAX).astype(jnp.int32)


def draw_block_counts(key, part):
    key_base, key_busy = jax.random.split(key)
    base_draw = jax.random.randint(key_base, (SECTIONS, REPLICAS), 1, KMAX // 2 + 1)
    busy_replica = jax.random.randint(key_busy, (SECTIONS, 1), 0, REPLICAS)
    placed = jnp.arange(REPLICAS, dtype=jnp.int32)[None, :] == busy_replica
    return jnp.where(placed, KMAX, base_draw).astype(jnp.int32)


def block_scale(stream_key, extent, cuts, low, top_value):
    level, own = 1.0, jax.random.fold_in(stream_key, 6)
    for axis_at, shards_of in cuts:
        draws = jnp.exp(jax.random.uniform(jax.random.fold_in(own, axis_at), (shards_of,), jnp.float32, low / len(cuts), top_value / len(cuts)))
        level = level * jnp.repeat(draws, extent[axis_at] // shards_of).reshape([-1 if axis == axis_at else 1 for axis in range(len(extent))])
    return level


def centred(rng, dims, scale, reach, shards=(), kind=jnp.bfloat16):
    array = scale * jax.random.normal(rng, dims, jnp.float32)
    if shards:
        array = array * block_scale(rng, dims, shards, -0.22, 0.18)
    return jnp.clip(array, -reach, reach).astype(kind)


def setup_inputs(seed: int = 0) -> dict:
    streams_of = jax.random.split(jax.random.key(seed), 5)
    gradient = draw_gradient(jax.random.fold_in(streams_of[4], 71), 0)
    residual = centred(streams_of[1], (SECTIONS * ROWS, REPLICAS * D), 1.0, 6.0, ((0, 4), (1, 8)), jnp.float32)
    block_ids = draw_block_ids(jax.random.fold_in(streams_of[4], 71), 0)
    block_counts = draw_block_counts(jax.random.fold_in(streams_of[4], 71), 0)
    return dict(gradient=gradient, residual=residual, block_ids=block_ids, block_counts=block_counts)


scale_level = 1.0
epsilon = 1e-06

def reference(gradient, residual, block_ids, block_counts):
    block_total = ROWS // BLK
    accumulated = gradient.astype(jnp.float32) + residual
    slot_ids = block_ids.reshape(SECTIONS, REPLICAS, KMAX)
    live_slot = jnp.arange(KMAX, dtype=jnp.int32)[None, None, :] < block_counts[:, :, None]
    hit_table = (slot_ids[..., None] == jnp.arange(block_total, dtype=jnp.int32)) & live_slot[..., None]
    chosen = jnp.any(hit_table, axis=2)
    block_mask = jnp.transpose(chosen, (0, 2, 1))[:, :, None, :, None]
    shaped = accumulated.reshape(SECTIONS, block_total, BLK, REPLICAS, D)
    sent = jnp.where(block_mask, shaped.astype(jnp.bfloat16).astype(jnp.float32), jnp.float32(0.0))
    new_residual = (shaped - sent).reshape(accumulated.shape)
    summed = lax.optimization_barrier(jnp.sum(sent, axis=3)).reshape(SECTIONS * ROWS, D)
    norm_total = jnp.sum(summed * summed)
    root_mean = jnp.sqrt(norm_total / (SECTIONS * ROWS * D) + epsilon)
    clip_factor = scale_level / root_mean
    update = (summed * clip_factor).astype(jnp.bfloat16)
    return (new_residual, update)
```

```python
import functools

import jax
import jax.numpy as jnp
from jax import lax
from jax.experimental import pallas as pl
from jax.experimental.pallas import tpu as pltpu
from jax.sharding import PartitionSpec as P

BLK = 8
CHUNKS = 4
LANES = 128
MESH = pl.DeviceIdType.MESH

scale_level = 1.0
epsilon = 1e-06


def kernel(
    sections,
    replicas,
    ids_hbm,
    counts_hbm,
    gradient_ref,
    residual_ref,
    update_ref,
    left_ref,
    grad_buf,
    acc_buf,
    packed,
    received,
    target_row,
    targets,
    square_row,
    squares,
    load_sems,
    ids_ref,
    counts_ref,
    list_sems,
    relayed,
    far_targets,
    far_data,
    cross_buf,
    cross_in,
    relay_sems,
    near_row_sems,
    near_sems,
    far_row_sems,
    far_sems,
    cross_sems,
    norm_send,
    norm_recv,
):
    row_count, width = gradient_ref.shape
    block_total = row_count // BLK
    slot_count = ids_hbm.shape[1]
    slot_rows = slot_count * BLK
    cap = slot_count // 2
    cap_rows = cap * BLK
    half = replicas // 2
    col_count = width // replicas
    section = lax.axis_index("section")
    replica = lax.axis_index("replica")
    total = sections * replicas

    def ahead(here, extent):
        return [here] + [
            jnp.where(here + k >= extent, here + k - extent, here + k) for k in range(1, extent)
        ]

    section_at = ahead(section, sections)
    replica_at = ahead(replica, replicas)
    others = [(i, j) for i in range(sections) for j in range(replicas) if i + j > 0]

    lists = [
        pltpu.make_async_copy(ids_hbm, ids_ref, list_sems.at[0]),
        pltpu.make_async_copy(counts_hbm, counts_ref, list_sems.at[1]),
    ]
    for copy in lists:
        copy.start()

    step = row_count // CHUNKS
    loads = []
    for c in range(CHUNKS):
        rows = pl.ds(c * step, step)
        blocks = pl.ds(c * step // BLK, step // BLK)
        one = pltpu.make_async_copy(gradient_ref.at[rows], grad_buf.at[rows], load_sems.at[0, c])
        two = pltpu.make_async_copy(residual_ref.at[blocks], acc_buf.at[blocks], load_sems.at[1, c])
        one.start()
        two.start()
        loads.append((one, two))

    barrier = pltpu.get_barrier_semaphore()

    greeted = [(i, j) for i, j in others if i == 0 or j == 0]
    for i, j in greeted:
        pl.semaphore_signal(
            barrier,
            inc=1,
            device_id={"section": section_at[i], "replica": replica_at[j]},
            device_id_type=MESH,
        )

    for copy in lists:
        copy.wait()
    lane = lax.broadcasted_iota(jnp.int32, (1, LANES), 1)
    row = jnp.full((1, LANES), -1, jnp.int32)
    for s in range(slot_count):
        base = jnp.where(s < counts_ref[0, 0], ids_ref[0, s] * BLK, -2 * row_count)
        row = jnp.where(lane // BLK == s, base + lane % BLK, row)
    target_row[...] = row

    for c in range(CHUNKS):
        for copy in loads[c]:
            copy.wait()
        rows = pl.ds(c * step, step)
        blocks = pl.ds(c * step // BLK, step // BLK)
        value = grad_buf[rows].astype(jnp.float32).reshape(step // BLK, BLK, width)
        acc_buf[blocks] = acc_buf[blocks] + value

    for s in range(0, slot_count, 2):
        pair = [acc_buf[ids_ref[0, s + i]] for i in range(2)]
        if s >= cap:
            pair = [jnp.where(s + i < counts_ref[0, 0], pair[i], 0.0) for i in range(2)]
        pair = jnp.concatenate(pair, axis=0).astype(jnp.bfloat16)
        for p in range(replicas):
            packed[p, pl.ds(s * BLK, 2 * BLK), :] = pair[:, p * col_count : (p + 1) * col_count]

    pl.semaphore_wait(barrier, len(greeted))

    side = replica // half * half
    other_side = half - side
    place_in_side = replica - side
    inner = [
        jnp.where(place_in_side + k >= half, place_in_side + k - half, place_in_side + k)
        for k in range(half)
    ]

    def send(src, dst, sems, slot, peer):
        copy = pltpu.make_async_remote_copy(
            src_ref=src,
            dst_ref=dst,
            send_sem=sems.at[0, slot],
            recv_sem=sems.at[1, slot],
            device_id={"replica": peer},
            device_id_type=MESH,
        )
        copy.start()
        return copy

    relay_in, near_rows, near, far_rows, far = {}, {}, {}, {}, {}
    for k in range(half - 1, 0, -1):
        peer = side + inner[k]
        source = packed.at[other_side + inner[k], pl.ds(cap_rows, slot_rows - cap_rows)]
        relay_in[k] = send(source, relayed.at[k - 1], relay_sems, k - 1, peer)
    for k in range(half - 1, -1, -1):
        peer = other_side + inner[k]
        far_rows[k] = send(target_row, far_targets.at[k], far_row_sems, k, peer)
        far[k] = send(packed.at[peer, pl.ds(0, cap_rows)], far_data.at[k], far_sems, k, peer)
    for k in range(half - 1, 0, -1):
        peer = side + inner[k]
        near_rows[k] = send(target_row, targets.at[k - 1], near_row_sems, k - 1, peer)
        near[k] = send(packed.at[peer], received.at[k - 1], near_sems, k - 1, peer)

    for c in range(CHUNKS):
        for b in range(c * step // BLK, (c + 1) * step // BLK):
            chosen = jnp.int32(0)
            for s in range(slot_count):
                hit = (ids_ref[0, s] == b) & (s < counts_ref[0, 0])
                chosen = jnp.where(hit, 1, chosen)
            value = acc_buf[b]
            rounded = value.astype(jnp.bfloat16).astype(jnp.float32)
            left_ref[b] = value - jnp.where(chosen > 0, rounded, 0.0)


    def place(wanted, block):
        row_iota = lax.broadcasted_iota(jnp.int32, (row_count, wanted.shape[1]), 0)
        hot = jnp.where(row_iota == wanted, 1.0, 0.0).astype(jnp.bfloat16)
        return jnp.dot(hot, block, preferred_element_type=jnp.float32)

    crossing = packed[other_side + place_in_side, cap_rows:, :].astype(jnp.float32)
    for k in range(1, half):
        relay_in[k].wait_recv()
        crossing = crossing + relayed[k - 1].astype(jnp.float32)
    cross_buf[...] = crossing.astype(jnp.bfloat16)
    cross = send(cross_buf, cross_in, cross_sems, 0, other_side + place_in_side)

    summed = place(target_row[:, :slot_rows], packed[replica])
    for k in range(1, half):
        near_rows[k].wait_recv()
        near[k].wait_recv()
        summed = summed + place(targets[k - 1][:, :slot_rows], received[k - 1])
    wanted = jnp.full((1, slot_rows), -1, jnp.int32)
    for k in range(half):
        far_rows[k].wait_recv()
        far[k].wait_recv()
        theirs = far_targets[k][:, :slot_rows]
        wanted = jnp.maximum(wanted, theirs)
        summed = summed + place(theirs[:, :cap_rows], far_data[k])
    cross.wait_recv()
    summed = summed + place(wanted[:, cap_rows:], cross_in[...])

    lanes = jnp.sum(summed * summed, axis=0, keepdims=True)
    part = lanes[:, :LANES]
    for j in range(1, col_count // LANES):
        part = part + lanes[:, j * LANES : (j + 1) * LANES]
    square_row[...] = part

    for slot, (i, j) in enumerate(others):
        pltpu.make_async_remote_copy(
            src_ref=square_row,
            dst_ref=squares.at[slot],
            send_sem=norm_send,
            recv_sem=norm_recv,
            device_id={"section": section_at[i], "replica": replica_at[j]},
            device_id_type=MESH,
        ).start()
    for group in (relay_in, near_rows, near, far_rows, far, {0: cross}):
        for copy in group.values():
            copy.wait_send()
    pltpu.make_async_copy(squares, squares, norm_recv).wait()
    pltpu.make_async_copy(squares, squares, norm_send).wait()
    norm_total = jnp.sum(part + jnp.sum(squares[...], axis=0), axis=1, keepdims=True)
    element_count = sections * row_count * width
    root_mean = jnp.sqrt(norm_total / element_count + epsilon)
    clip_factor = scale_level / root_mean
    update_ref[...] = (summed * clip_factor).astype(jnp.bfloat16)


def finish(update_ref, left_ref, update_out, left_out, sems):
    copies = [pltpu.make_async_copy(update_ref, update_out, sems.at[0])]
    parts = left_ref.shape[0] // CHUNKS
    for c in range(CHUNKS):
        part = pl.ds(c * parts, parts)
        copies.append(pltpu.make_async_copy(left_ref.at[part], left_out.at[part], sems.at[c + 1]))
    for copy in copies:
        copy.start()
    for copy in copies:
        copy.wait()


def per_device(sections, replicas, gradient, residual, block_ids, block_counts):
    row_count, width = gradient.shape
    block_total = row_count // BLK
    slot_count = block_ids.shape[1]
    col_count = width // replicas
    total = sections * replicas
    slot_rows = slot_count * BLK
    over_rows = slot_rows - slot_count // 2 * BLK
    half = replicas // 2
    update, left = pl.pallas_call(
        functools.partial(kernel, sections, replicas),
        out_shape=(
            pltpu.VMEM((row_count, col_count), jnp.bfloat16),
            pltpu.VMEM((block_total, BLK, width), jnp.float32),
        ),
        in_specs=[
            pl.BlockSpec(memory_space=pltpu.HBM),
            pl.BlockSpec(memory_space=pltpu.HBM),
            pl.BlockSpec(memory_space=pltpu.HBM),
            pl.BlockSpec(memory_space=pltpu.HBM),
        ],
        out_specs=(
            pl.BlockSpec(memory_space=pltpu.VMEM),
            pl.BlockSpec(memory_space=pltpu.VMEM),
        ),
        scratch_shapes=[
            pltpu.VMEM((row_count, width), jnp.bfloat16),
            pltpu.VMEM((block_total, BLK, width), jnp.float32),
            pltpu.VMEM((replicas, slot_rows, col_count), jnp.bfloat16),
            pltpu.VMEM((half - 1, slot_rows, col_count), jnp.bfloat16),
            pltpu.VMEM((1, LANES), jnp.int32),
            pltpu.VMEM((half - 1, 1, LANES), jnp.int32),
            pltpu.VMEM((1, LANES), jnp.float32),
            pltpu.VMEM((total - 1, 1, LANES), jnp.float32),
            pltpu.SemaphoreType.DMA((2, CHUNKS)),
            pltpu.SMEM(block_ids.shape, jnp.int32),
            pltpu.SMEM(block_counts.shape, jnp.int32),
            pltpu.SemaphoreType.DMA((2,)),
            pltpu.VMEM((half - 1, over_rows, col_count), jnp.bfloat16),
            pltpu.VMEM((half, 1, LANES), jnp.int32),
            pltpu.VMEM((half, slot_rows - over_rows, col_count), jnp.bfloat16),
            pltpu.VMEM((over_rows, col_count), jnp.bfloat16),
            pltpu.VMEM((over_rows, col_count), jnp.bfloat16),
            pltpu.SemaphoreType.DMA((2, half - 1)),
            pltpu.SemaphoreType.DMA((2, half - 1)),
            pltpu.SemaphoreType.DMA((2, half - 1)),
            pltpu.SemaphoreType.DMA((2, half)),
            pltpu.SemaphoreType.DMA((2, half)),
            pltpu.SemaphoreType.DMA((2, 1)),
            pltpu.SemaphoreType.DMA,
            pltpu.SemaphoreType.DMA,
        ],
        compiler_params=pltpu.CompilerParams(collective_id=0, has_side_effects=True),
    )(block_ids, block_counts, gradient, residual.reshape(block_total, BLK, width))

    update, left = pl.pallas_call(
        finish,
        out_shape=(
            jax.ShapeDtypeStruct(update.shape, update.dtype),
            jax.ShapeDtypeStruct(left.shape, left.dtype),
        ),
        in_specs=[pl.BlockSpec(memory_space=pltpu.VMEM)] * 2,
        out_specs=(pl.BlockSpec(memory_space=pltpu.HBM),) * 2,
        scratch_shapes=[pltpu.SemaphoreType.DMA((CHUNKS + 1,))],
        compiler_params=pltpu.CompilerParams(vmem_limit_bytes=1 << 20),
    )(update, left)
    return (left.reshape(row_count, width), update)


def solution(mesh):
    spec = P("section", "replica")
    sizes = (mesh.shape["section"], mesh.shape["replica"])
    return jax.shard_map(
        functools.partial(per_device, *sizes),
        mesh=mesh,
        in_specs=(spec,) * 4,
        out_specs=(spec, spec),
        check_vma=False,
    )
```

```python
import functools

import jax
import jax.numpy as jnp
from jax import lax
from jax.experimental import pallas as pl
from jax.experimental.pallas import tpu as pltpu
from jax.sharding import PartitionSpec as P

BLK = 8
LANES = 128
EARLY_STEPS = 8
MESH = pl.DeviceIdType.MESH

scale_level = 1.0
epsilon = 1e-06


def flip(index, mask):
    bit, out = 1, index
    while bit <= mask:
        if mask & bit:
            out = out + bit - 2 * bit * (index // bit % 2)
        bit *= 2
    return out


def exchange(
    sections,
    replicas,
    ids_hbm,
    counts_hbm,
    gradient_hbm,
    residual_hbm,
    early_hbm,
    update_ref,
    left_ref,
    grad_buf,
    res_buf,
    packed,
    target_row,
    ids_ref,
    counts_ref,
    list_sems,
    load_sems,
    ready,
    relayed,
    near_rows_buf,
    near_buf,
    far_rows_buf,
    far_buf,
    cross_buf,
    cross_in,
    relay_sems,
    near_row_sems,
    near_sems,
    far_row_sems,
    far_sems,
    cross_sems,
    square_row,
    squares,
    norm_send,
    norm_recv,
):
    block_total, _, width = residual_hbm.shape
    row_count = block_total * BLK
    slot_count = ids_hbm.shape[1]
    slot_rows = slot_count * BLK
    cap = slot_count // 2
    cap_rows = cap * BLK
    half = replicas // 2
    col_count = width // replicas
    section = lax.axis_index("section")
    replica = lax.axis_index("replica")

    def ahead(here, extent):
        return [here] + [
            jnp.where(here + k >= extent, here + k - extent, here + k) for k in range(1, extent)
        ]

    section_at = ahead(section, sections)
    peer_at = [flip(replica, mask) for mask in range(replicas)]
    others = [(i, j) for i in range(sections) for j in range(replicas) if i + j > 0]

    quarter = replicas // 4
    part_at = replica // quarter
    lower = part_at < 2
    inner = (part_at == 1) | (part_at == 2)
    beside = [half + quarter + low for low in range(quarter)]
    beyond = [half + low for low in range(quarter)]

    def greet(i, j):
        pl.semaphore_signal(
            barrier,
            inc=1,
            device_id={"section": section_at[i], "replica": peer_at[j]},
            device_id_type=MESH,
        )

    barrier = pltpu.get_barrier_semaphore()
    for j in range(1, half):
        greet(0, j)
    for i in range(1, sections):
        greet(i, 0)
    for j in beside:
        pl.when(lower | inner)(functools.partial(greet, 0, j))
    for j in beyond:
        pl.when(lower | (part_at == 3))(functools.partial(greet, 0, j))
    greeted = half - 1 + sections - 1 + jnp.where(part_at == 0, 0, half)

    lists = [
        pltpu.make_async_copy(ids_hbm, ids_ref, list_sems.at[0]),
        pltpu.make_async_copy(counts_hbm, counts_ref, list_sems.at[1]),
    ]
    for copy in lists:
        copy.start()

    order = list(range(replicas - 1, -1, -1))
    same = list(range(1, quarter))
    next_to = list(range(quarter, half))
    loads = {}
    for mask in order:
        cols = pl.ds(pl.multiple_of(peer_at[mask] * col_count, col_count), col_count)
        loads[mask] = (
            pltpu.make_async_copy(gradient_hbm.at[:, :, cols], grad_buf[mask], load_sems.at[0, mask]),
            pltpu.make_async_copy(residual_hbm.at[:, :, cols], res_buf[mask], load_sems.at[1, mask]),
        )
        for copy in loads[mask]:
            copy.start()

    for copy in lists:
        copy.wait()
    count = counts_ref[0, 0]
    ids = [ids_ref[0, s] for s in range(slot_count)]
    lane = lax.broadcasted_iota(jnp.int32, (1, LANES), 1)
    row = jnp.full((1, LANES), -1, jnp.int32)
    for s in range(slot_count):
        base = jnp.where(s < count, ids[s] * BLK, -2 * row_count)
        row = jnp.where(lane // BLK == s, base + lane % BLK, row)
    target_row[...] = row

    def pack(mask):
        for copy in loads[mask]:
            copy.wait()
        for s in range(0, slot_count, 2):
            pair = []
            for i in (s, s + 1):
                value = grad_buf[mask][ids[i]].astype(jnp.float32) + res_buf[mask][ids[i]]
                if s >= cap:
                    value = jnp.where(i < count, value, 0.0)
                pair.append(value)
            packed[mask, pl.ds(s * BLK, 2 * BLK), :] = jnp.concatenate(pair, axis=0).astype(jnp.bfloat16)

    def make(src, dst, sems, slot, peer):
        return pltpu.make_async_remote_copy(
            src_ref=src,
            dst_ref=dst,
            send_sem=sems.at[0, slot],
            recv_sem=sems.at[1, slot],
            device_id={"replica": peer},
            device_id_type=MESH,
        )

    relay_in, near_rows, near, far_rows, far = {}, {}, {}, {}, {}
    for mask in range(1, half):
        peer = peer_at[mask]
        relay_in[mask] = make(
            packed.at[half + mask, pl.ds(cap_rows, slot_rows - cap_rows)],
            relayed.at[mask - 1],
            relay_sems,
            mask - 1,
            peer,
        )
        near_rows[mask] = make(target_row, near_rows_buf.at[mask - 1], near_row_sems, mask - 1, peer)
        near[mask] = make(packed.at[mask], near_buf.at[mask - 1], near_sems, mask - 1, peer)
    for mask in range(half, replicas):
        peer, slot = peer_at[mask], mask - half
        far_rows[mask] = make(target_row, far_rows_buf.at[slot], far_row_sems, slot, peer)
        far[mask] = make(packed.at[mask, pl.ds(0, cap_rows)], far_buf.at[slot], far_sems, slot, peer)
    cross = make(cross_buf, cross_in, cross_sems, 0, peer_at[half])

    def start_far(masks):
        for mask in masks:
            far_rows[mask].start()
            far[mask].start()

    def tell(mask):
        pl.semaphore_signal(ready, inc=1, device_id={"replica": peer_at[mask]}, device_id_type=MESH)

    def start_near(masks):
        for mask in masks[::-1]:
            near_rows[mask].start()
            near[mask].start()

    for mask in order[: half - 1]:
        pack(mask)
    pl.semaphore_wait(barrier, greeted)
    pl.when(part_at == 1)(functools.partial(tell, quarter))
    for mask in range(half - 1, 0, -1):
        relay_in[mask].start()
    pl.when(inner)(functools.partial(start_far, beside))
    pack(half)
    pl.when(inner)(functools.partial(start_far, beyond))
    for mask in order[half:]:
        pack(mask)
    for mask in range(half - 1, 0, -1):
        relay_in[mask].wait_send()

    @pl.when(part_at == 3)
    def _():
        start_far(beside)
        start_far(beyond)

    start_near(next_to)
    start_near(same)

    @pl.when(part_at == 0)
    def _():
        pl.semaphore_wait(ready, 1)
        start_far(beside)
        start_far(beyond)

    for b in range(block_total):
        chosen = jnp.int32(0)
        for s in range(slot_count):
            chosen = jnp.where((ids[s] == b) & (s < count), 1, chosen)
        for mask in order:
            value = grad_buf[mask][b].astype(jnp.float32) + res_buf[mask][b]
            rounded = value.astype(jnp.bfloat16).astype(jnp.float32)
            left_ref[mask, b] = value - jnp.where(chosen > 0, rounded, 0.0)

    def place(wanted, block):
        row_iota = lax.broadcasted_iota(jnp.int32, (row_count, wanted.shape[1]), 0)
        hot = jnp.where(row_iota == wanted, 1.0, 0.0).astype(jnp.bfloat16)
        return jnp.dot(hot, block, preferred_element_type=jnp.float32)

    crossing = packed[half, cap_rows:, :].astype(jnp.float32)
    for mask in range(half - 1, 0, -1):
        relay_in[mask].wait_recv()
        crossing = crossing + relayed[mask - 1].astype(jnp.float32)
    cross_buf[...] = crossing.astype(jnp.bfloat16)
    cross.start()

    summed = place(target_row[:, :slot_rows], packed[0])
    for mask in range(half - 1, 0, -1):
        near_rows[mask].wait_recv()
        near[mask].wait_recv()
        summed = summed + place(near_rows_buf[mask - 1][:, :slot_rows], near_buf[mask - 1])
    wanted = jnp.full((1, slot_rows), -1, jnp.int32)
    for mask in range(replicas - 1, half - 1, -1):
        far_rows[mask].wait_recv()
        far[mask].wait_recv()
        theirs = far_rows_buf[mask - half][:, :slot_rows]
        wanted = jnp.maximum(wanted, theirs)
        summed = summed + place(theirs[:, :cap_rows], far_buf[mask - half])
    cross.wait_recv()
    summed = summed + place(wanted[:, cap_rows:], cross_in[...])

    lanes = jnp.sum(summed * summed, axis=0, keepdims=True)
    part = lanes[:, :LANES]
    for j in range(1, col_count // LANES):
        part = part + lanes[:, j * LANES : (j + 1) * LANES]
    square_row[...] = part

    for slot, (i, j) in reversed(list(enumerate(others))):
        pltpu.make_async_remote_copy(
            src_ref=square_row,
            dst_ref=squares.at[slot],
            send_sem=norm_send,
            recv_sem=norm_recv,
            device_id={"section": section_at[i], "replica": peer_at[j]},
            device_id_type=MESH,
        ).start()
    for group in (near_rows, near, far_rows, far, {0: cross}):
        for copy in group.values():
            copy.wait_send()
    pltpu.make_async_copy(squares, squares, norm_recv).wait()
    pltpu.make_async_copy(squares, squares, norm_send).wait()
    norm_total = jnp.sum(part + jnp.sum(squares[...], axis=0), axis=1, keepdims=True)
    element_count = sections * row_count * width
    root_mean = jnp.sqrt(norm_total / element_count + epsilon)
    clip_factor = scale_level / root_mean
    update_ref[...] = (summed * clip_factor).astype(jnp.bfloat16)


def residual_early(early, ids_hbm, counts_hbm, gradient_hbm, residual_hbm, left_hbm, *scratch):
    grad_buf, res_buf, ids_ref, counts_ref, list_sems, load_sems, out_sems = scratch
    block_total = residual_hbm.shape[0]
    slot_count = ids_hbm.shape[1]
    step = block_total // EARLY_STEPS

    @pl.when(early())
    def _():
        lists = [
            pltpu.make_async_copy(ids_hbm, ids_ref, list_sems.at[0]),
            pltpu.make_async_copy(counts_hbm, counts_ref, list_sems.at[1]),
        ]
        for copy in lists:
            copy.start()
        loads, stores = [], []
        for c in range(EARLY_STEPS):
            part = pl.ds(c * step, step)
            loads.append(
                (
                    pltpu.make_async_copy(gradient_hbm.at[part], grad_buf.at[part], load_sems.at[0, c]),
                    pltpu.make_async_copy(residual_hbm.at[part], res_buf.at[part], load_sems.at[1, c]),
                )
            )
            stores.append(pltpu.make_async_copy(res_buf.at[part], left_hbm.at[part], out_sems.at[c]))
            for copy in loads[c]:
                copy.start()
        for copy in lists:
            copy.wait()
        for c in range(EARLY_STEPS):
            for copy in loads[c]:
                copy.wait()
            for b in range(c * step, (c + 1) * step):
                chosen = jnp.int32(0)
                for s in range(slot_count):
                    chosen = jnp.where((ids_ref[0, s] == b) & (s < counts_ref[0, 0]), 1, chosen)
                value = grad_buf[b].astype(jnp.float32) + res_buf[b]
                rounded = value.astype(jnp.bfloat16).astype(jnp.float32)
                res_buf[b] = value - jnp.where(chosen > 0, rounded, 0.0)
            stores[c].start()
        for copy in stores:
            copy.wait()


def starts_early():
    return (lax.axis_index("replica") == 0) & (lax.axis_index("section") < 2)


def deliver(replicas, early, update_ref, left_ref, early_hbm, update_hbm, left_hbm, sems):
    col_count = left_ref.shape[3]
    replica = lax.axis_index("replica")
    update_copy = pltpu.make_async_copy(update_ref, update_hbm, sems.at[replicas])
    update_copy.start()

    @pl.when(jnp.logical_not(early()))
    def _():
        copies = []
        for mask in range(replicas):
            cols = pl.ds(pl.multiple_of(flip(replica, mask) * col_count, col_count), col_count)
            copies.append(pltpu.make_async_copy(left_ref.at[mask], left_hbm.at[:, :, cols], sems.at[mask]))
        for copy in copies:
            copy.start()
        for copy in copies:
            copy.wait()

    update_copy.wait()


def per_device(sections, replicas, gradient, residual, block_ids, block_counts):
    row_count, width = gradient.shape
    block_total = row_count // BLK
    slot_count = block_ids.shape[1]
    col_count = width // replicas
    total = sections * replicas
    slot_rows = slot_count * BLK
    cap_rows = slot_count // 2 * BLK
    over_rows = slot_rows - cap_rows
    half = replicas // 2
    pair = pltpu.SemaphoreType.DMA
    gradient = gradient.reshape(block_total, BLK, width)
    residual = residual.reshape(block_total, BLK, width)
    early = pl.pallas_call(
        functools.partial(residual_early, starts_early),
        out_shape=jax.ShapeDtypeStruct(residual.shape, residual.dtype),
        in_specs=[pl.BlockSpec(memory_space=pl.ANY)] * 4,
        out_specs=pl.BlockSpec(memory_space=pltpu.HBM),
        scratch_shapes=[
            pltpu.VMEM(gradient.shape, gradient.dtype),
            pltpu.VMEM(residual.shape, residual.dtype),
            pltpu.SMEM(block_ids.shape, jnp.int32),
            pltpu.SMEM(block_counts.shape, jnp.int32),
            pair((2,)),
            pair((2, EARLY_STEPS)),
            pair((EARLY_STEPS,)),
        ],
    )(block_ids, block_counts, gradient, residual)
    update, left = pl.pallas_call(
        functools.partial(exchange, sections, replicas),
        out_shape=(
            pltpu.VMEM((row_count, col_count), jnp.bfloat16),
            pltpu.VMEM((replicas, block_total, BLK, col_count), jnp.float32),
        ),
        in_specs=[pl.BlockSpec(memory_space=pl.ANY)] * 5,
        out_specs=(pl.BlockSpec(memory_space=pltpu.VMEM),) * 2,
        scratch_shapes=[
            [pltpu.VMEM((block_total, BLK, col_count), jnp.bfloat16)] * replicas,
            [pltpu.VMEM((block_total, BLK, col_count), jnp.float32)] * replicas,
            pltpu.VMEM((replicas, slot_rows, col_count), jnp.bfloat16),
            pltpu.VMEM((1, LANES), jnp.int32),
            pltpu.SMEM(block_ids.shape, jnp.int32),
            pltpu.SMEM(block_counts.shape, jnp.int32),
            pair((2,)),
            pair((2, replicas)),
            pltpu.SemaphoreType.REGULAR,
            pltpu.VMEM((half - 1, over_rows, col_count), jnp.bfloat16),
            pltpu.VMEM((half - 1, 1, LANES), jnp.int32),
            pltpu.VMEM((half - 1, slot_rows, col_count), jnp.bfloat16),
            pltpu.VMEM((half, 1, LANES), jnp.int32),
            pltpu.VMEM((half, cap_rows, col_count), jnp.bfloat16),
            pltpu.VMEM((over_rows, col_count), jnp.bfloat16),
            pltpu.VMEM((over_rows, col_count), jnp.bfloat16),
            pair((2, half - 1)),
            pair((2, half - 1)),
            pair((2, half - 1)),
            pair((2, half)),
            pair((2, half)),
            pair((2, 1)),
            pltpu.VMEM((1, LANES), jnp.float32),
            pltpu.VMEM((total - 1, 1, LANES), jnp.float32),
            pltpu.SemaphoreType.DMA,
            pltpu.SemaphoreType.DMA,
        ],
        compiler_params=pltpu.CompilerParams(collective_id=0, has_side_effects=True),
    )(
        block_ids,
        block_counts,
        gradient,
        residual,
        early,
    )
    update, left = pl.pallas_call(
        functools.partial(deliver, replicas, starts_early),
        out_shape=(
            jax.ShapeDtypeStruct(update.shape, update.dtype),
            jax.ShapeDtypeStruct((block_total, BLK, width), left.dtype),
        ),
        in_specs=[pl.BlockSpec(memory_space=pl.ANY)] * 2 + [pl.BlockSpec(memory_space=pltpu.HBM)],
        out_specs=(pl.BlockSpec(memory_space=pltpu.HBM),) * 2,
        input_output_aliases={2: 1},
        scratch_shapes=[pltpu.SemaphoreType.DMA((replicas + 1,))],
        compiler_params=pltpu.CompilerParams(vmem_limit_bytes=1 << 20),
    )(update, left, early)
    return (left.reshape(row_count, width), update)


def solution(mesh):
    spec = P("section", "replica")
    sizes = (mesh.shape["section"], mesh.shape["replica"])
    return jax.shard_map(
        functools.partial(per_device, *sizes),
        mesh=mesh,
        in_specs=(spec,) * 4,
        out_specs=(spec, spec),
        check_vma=False,
    )
```

```python
import functools

import jax
import jax.numpy as jnp
from jax import lax
from jax.experimental import pallas as pl
from jax.experimental.pallas import tpu as pltpu
from jax.sharding import PartitionSpec as P

BLK = 8
LANES = 128
EARLY_STEPS = 8
MESH = pl.DeviceIdType.MESH

scale_level = 1.0
epsilon = 1e-06


def flip(index, mask):
    bit, out = 1, index
    while bit <= mask:
        if mask & bit:
            out = out + bit - 2 * bit * (index // bit % 2)
        bit *= 2
    return out


def exchange(
    sections,
    replicas,
    ids_hbm,
    counts_hbm,
    gradient_hbm,
    residual_hbm,
    early_hbm,
    update_ref,
    left_ref,
    grad_buf,
    res_buf,
    packed,
    target_row,
    ids_ref,
    counts_ref,
    list_sems,
    load_sems,
    ready,
    relayed,
    near_rows_buf,
    near_buf,
    far_rows_buf,
    far_buf,
    cross_buf,
    cross_in,
    relay_sems,
    near_row_sems,
    near_sems,
    far_row_sems,
    far_sems,
    cross_sems,
    mate_buf,
    over_buf,
    near_over,
    mate_sems,
    over_sems,
    square_row,
    squares,
    norm_send,
    norm_recv,
):
    block_total, _, width = residual_hbm.shape
    row_count = block_total * BLK
    slot_count = ids_hbm.shape[1]
    slot_rows = slot_count * BLK
    cap = slot_count // 2
    cap_rows = cap * BLK
    half = replicas // 2
    col_count = width // replicas
    section = lax.axis_index("section")
    replica = lax.axis_index("replica")

    def ahead(here, extent):
        return [here] + [
            jnp.where(here + k >= extent, here + k - extent, here + k) for k in range(1, extent)
        ]

    section_at = ahead(section, sections)
    peer_at = [flip(replica, mask) for mask in range(replicas)]
    others = [(i, j) for i in range(sections) for j in range(replicas) if i + j > 0]

    quarter = replicas // 4
    part_at = replica // quarter
    lower = part_at < 2
    inner = (part_at == 1) | (part_at == 2)
    beside = [half + quarter + low for low in range(quarter)]
    beyond = [half + low for low in range(quarter)]

    def greet(i, j):
        pl.semaphore_signal(
            barrier,
            inc=1,
            device_id={"section": section_at[i], "replica": peer_at[j]},
            device_id_type=MESH,
        )

    barrier = pltpu.get_barrier_semaphore()
    for j in range(1, half):
        greet(0, j)
    for i in range(1, sections):
        greet(i, 0)
    for j in beside:
        pl.when(lower | inner)(functools.partial(greet, 0, j))
    for j in beyond:
        pl.when(lower | (part_at == 3))(functools.partial(greet, 0, j))
    greeted = half - 1 + sections - 1 + jnp.where(part_at == 0, 0, half)

    lists = [
        pltpu.make_async_copy(ids_hbm, ids_ref, list_sems.at[0]),
        pltpu.make_async_copy(counts_hbm, counts_ref, list_sems.at[1]),
    ]
    for copy in lists:
        copy.start()

    order = list(range(replicas - 1, -1, -1))
    same = list(range(1, quarter))
    next_to = list(range(quarter, half))
    loads = {}
    for mask in order:
        cols = pl.ds(pl.multiple_of(peer_at[mask] * col_count, col_count), col_count)
        loads[mask] = (
            pltpu.make_async_copy(gradient_hbm.at[:, :, cols], grad_buf[mask], load_sems.at[0, mask]),
            pltpu.make_async_copy(residual_hbm.at[:, :, cols], res_buf[mask], load_sems.at[1, mask]),
        )
        for copy in loads[mask]:
            copy.start()

    for copy in lists:
        copy.wait()
    count = counts_ref[0, 0]
    ids = [ids_ref[0, s] for s in range(slot_count)]
    lane = lax.broadcasted_iota(jnp.int32, (1, LANES), 1)
    row = jnp.full((1, LANES), -1, jnp.int32)
    for s in range(slot_count):
        base = jnp.where(s < count, ids[s] * BLK, -2 * row_count)
        row = jnp.where(lane // BLK == s, base + lane % BLK, row)
    target_row[...] = row

    def pack(mask):
        for copy in loads[mask]:
            copy.wait()
        for s in range(0, slot_count, 2):
            pair = []
            for i in (s, s + 1):
                value = grad_buf[mask][ids[i]].astype(jnp.float32) + res_buf[mask][ids[i]]
                if s >= cap:
                    value = jnp.where(i < count, value, 0.0)
                pair.append(value)
            packed[mask, pl.ds(s * BLK, 2 * BLK), :] = jnp.concatenate(pair, axis=0).astype(jnp.bfloat16)

    def make(src, dst, sems, slot, peer):
        return pltpu.make_async_remote_copy(
            src_ref=src,
            dst_ref=dst,
            send_sem=sems.at[0, slot],
            recv_sem=sems.at[1, slot],
            device_id={"replica": peer},
            device_id_type=MESH,
        )

    relay_in, near_rows, near, far_rows, far = {}, {}, {}, {}, {}
    for mask in range(1, half):
        peer = peer_at[mask]
        relay_in[mask] = make(
            packed.at[half + mask, pl.ds(cap_rows, slot_rows - cap_rows)],
            relayed.at[mask - 1],
            relay_sems,
            mask - 1,
            peer,
        )
        near_rows[mask] = make(target_row, near_rows_buf.at[mask - 1], near_row_sems, mask - 1, peer)
        rows = pl.ds(0, slot_rows if mask in same else cap_rows)
        near[mask] = make(packed.at[mask, rows], near_buf.at[mask - 1, rows], near_sems, mask - 1, peer)
    for mask in range(half, replicas):
        peer, slot = peer_at[mask], mask - half
        far_rows[mask] = make(target_row, far_rows_buf.at[slot], far_row_sems, slot, peer)
        far[mask] = make(packed.at[mask, pl.ds(0, cap_rows)], far_buf.at[slot], far_sems, slot, peer)
    mate = {}
    for mask in same:
        mate[mask] = make(
            packed.at[quarter + mask, pl.ds(cap_rows, slot_rows - cap_rows)],
            mate_buf.at[mask - 1],
            mate_sems,
            mask - 1,
            peer_at[mask],
        )
    over = make(over_buf, near_over, over_sems, 0, peer_at[quarter])
    cross = make(cross_buf, cross_in, cross_sems, 0, peer_at[half])

    def start_far(masks):
        for mask in masks:
            far_rows[mask].start()
            far[mask].start()

    def tell(mask):
        pl.semaphore_signal(ready, inc=1, device_id={"replica": peer_at[mask]}, device_id_type=MESH)

    def start_near(masks):
        for mask in masks:
            near_rows[mask].start()
            near[mask].start()

    urgent = order[: half - 1]
    for mask in urgent:
        pack(mask)
    pl.semaphore_wait(barrier, greeted)
    pl.when(part_at == 1)(functools.partial(tell, quarter))
    for mask in next_to[::-1] + same:
        relay_in[mask].start()
    pl.when(inner)(functools.partial(start_far, beside))
    pack(half)
    pl.when(inner)(functools.partial(start_far, beyond[::-1]))
    for mask in order[half:]:
        if mask not in urgent:
            pack(mask)
    for mask in same:
        mate[mask].start()
    @pl.when(part_at == 3)
    def _():
        start_far(beyond[::-1])
        start_far(beside)

    for mask in range(half - 1, 0, -1):
        relay_in[mask].wait_send()

    @pl.when(part_at == 0)
    def _():
        pl.semaphore_wait(ready, 1)
        start_far(beside)
        start_far(beyond[::-1])

    start_near(next_to[::-1] + same)

    for b in range(block_total):
        chosen = jnp.int32(0)
        for s in range(slot_count):
            chosen = jnp.where((ids[s] == b) & (s < count), 1, chosen)
        for mask in order:
            value = grad_buf[mask][b].astype(jnp.float32) + res_buf[mask][b]
            rounded = value.astype(jnp.bfloat16).astype(jnp.float32)
            left_ref[mask, b] = value - jnp.where(chosen > 0, rounded, 0.0)

    def place(wanted, block):
        row_iota = lax.broadcasted_iota(jnp.int32, (row_count, wanted.shape[1]), 0)
        hot = jnp.where(row_iota == wanted, 1.0, 0.0).astype(jnp.bfloat16)
        return jnp.dot(hot, block, preferred_element_type=jnp.float32)

    crossing = packed[half, cap_rows:, :].astype(jnp.float32)
    for mask in range(half - 1, 0, -1):
        relay_in[mask].wait_recv()
        crossing = crossing + relayed[mask - 1].astype(jnp.float32)
    cross_buf[...] = crossing.astype(jnp.bfloat16)
    cross.start()
    beside_over = packed[quarter, cap_rows:, :].astype(jnp.float32)
    for mask in same:
        mate[mask].wait_recv()
        beside_over = beside_over + mate_buf[mask - 1].astype(jnp.float32)
    over_buf[...] = beside_over.astype(jnp.bfloat16)
    over.start()

    summed = place(target_row[:, :slot_rows], packed[0])
    wanted = jnp.full((1, slot_rows), -1, jnp.int32)
    for mask in range(half - 1, 0, -1):
        near_rows[mask].wait_recv()
        near[mask].wait_recv()
        theirs = near_rows_buf[mask - 1][:, :slot_rows]
        if mask in same:
            summed = summed + place(theirs, near_buf[mask - 1])
        else:
            wanted = jnp.maximum(wanted, theirs)
            summed = summed + place(theirs[:, :cap_rows], near_buf[mask - 1, :cap_rows])
    over.wait_recv()
    summed = summed + place(wanted[:, cap_rows:], near_over[...])
    wanted = jnp.full((1, slot_rows), -1, jnp.int32)
    for mask in range(replicas - 1, half - 1, -1):
        far_rows[mask].wait_recv()
        far[mask].wait_recv()
        theirs = far_rows_buf[mask - half][:, :slot_rows]
        wanted = jnp.maximum(wanted, theirs)
        summed = summed + place(theirs[:, :cap_rows], far_buf[mask - half])
    cross.wait_recv()
    summed = summed + place(wanted[:, cap_rows:], cross_in[...])

    lanes = jnp.sum(summed * summed, axis=0, keepdims=True)
    part = lanes[:, :LANES]
    for j in range(1, col_count // LANES):
        part = part + lanes[:, j * LANES : (j + 1) * LANES]
    square_row[...] = part

    for slot, (i, j) in reversed(list(enumerate(others))):
        pltpu.make_async_remote_copy(
            src_ref=square_row,
            dst_ref=squares.at[slot],
            send_sem=norm_send,
            recv_sem=norm_recv,
            device_id={"section": section_at[i], "replica": peer_at[j]},
            device_id_type=MESH,
        ).start()
    for group in (near_rows, near, far_rows, far, mate, {0: cross, 1: over}):
        for copy in group.values():
            copy.wait_send()
    pltpu.make_async_copy(squares, squares, norm_recv).wait()
    pltpu.make_async_copy(squares, squares, norm_send).wait()
    norm_total = jnp.sum(part + jnp.sum(squares[...], axis=0), axis=1, keepdims=True)
    element_count = sections * row_count * width
    root_mean = jnp.sqrt(norm_total / element_count + epsilon)
    clip_factor = scale_level / root_mean
    update_ref[...] = (summed * clip_factor).astype(jnp.bfloat16)


def residual_early(early, ids_hbm, counts_hbm, gradient_hbm, residual_hbm, left_hbm, *scratch):
    grad_buf, res_buf, ids_ref, counts_ref, list_sems, load_sems, out_sems = scratch
    block_total = residual_hbm.shape[0]
    slot_count = ids_hbm.shape[1]
    step = block_total // EARLY_STEPS

    @pl.when(early())
    def _():
        lists = [
            pltpu.make_async_copy(ids_hbm, ids_ref, list_sems.at[0]),
            pltpu.make_async_copy(counts_hbm, counts_ref, list_sems.at[1]),
        ]
        for copy in lists:
            copy.start()
        loads, stores = [], []
        for c in range(EARLY_STEPS):
            part = pl.ds(c * step, step)
            loads.append(
                (
                    pltpu.make_async_copy(gradient_hbm.at[part], grad_buf.at[part], load_sems.at[0, c]),
                    pltpu.make_async_copy(residual_hbm.at[part], res_buf.at[part], load_sems.at[1, c]),
                )
            )
            stores.append(pltpu.make_async_copy(res_buf.at[part], left_hbm.at[part], out_sems.at[c]))
            for copy in loads[c]:
                copy.start()
        for copy in lists:
            copy.wait()
        for c in range(EARLY_STEPS):
            for copy in loads[c]:
                copy.wait()
            for b in range(c * step, (c + 1) * step):
                chosen = jnp.int32(0)
                for s in range(slot_count):
                    chosen = jnp.where((ids_ref[0, s] == b) & (s < counts_ref[0, 0]), 1, chosen)
                value = grad_buf[b].astype(jnp.float32) + res_buf[b]
                rounded = value.astype(jnp.bfloat16).astype(jnp.float32)
                res_buf[b] = value - jnp.where(chosen > 0, rounded, 0.0)
            stores[c].start()
        for copy in stores:
            copy.wait()


def starts_early():
    return (lax.axis_index("replica") == 0) & (lax.axis_index("section") < 2)


def deliver(replicas, early, update_ref, left_ref, early_hbm, update_hbm, left_hbm, sems):
    col_count = left_ref.shape[3]
    replica = lax.axis_index("replica")
    update_copy = pltpu.make_async_copy(update_ref, update_hbm, sems.at[replicas])
    update_copy.start()

    @pl.when(jnp.logical_not(early()))
    def _():
        copies = []
        for mask in range(replicas):
            cols = pl.ds(pl.multiple_of(flip(replica, mask) * col_count, col_count), col_count)
            copies.append(pltpu.make_async_copy(left_ref.at[mask], left_hbm.at[:, :, cols], sems.at[mask]))
        for copy in copies:
            copy.start()
        for copy in copies:
            copy.wait()

    update_copy.wait()


def per_device(sections, replicas, gradient, residual, block_ids, block_counts):
    row_count, width = gradient.shape
    block_total = row_count // BLK
    slot_count = block_ids.shape[1]
    col_count = width // replicas
    total = sections * replicas
    slot_rows = slot_count * BLK
    cap_rows = slot_count // 2 * BLK
    over_rows = slot_rows - cap_rows
    half = replicas // 2
    pair = pltpu.SemaphoreType.DMA
    gradient = gradient.reshape(block_total, BLK, width)
    residual = residual.reshape(block_total, BLK, width)
    early = pl.pallas_call(
        functools.partial(residual_early, starts_early),
        out_shape=jax.ShapeDtypeStruct(residual.shape, residual.dtype),
        in_specs=[pl.BlockSpec(memory_space=pl.ANY)] * 4,
        out_specs=pl.BlockSpec(memory_space=pltpu.HBM),
        scratch_shapes=[
            pltpu.VMEM(gradient.shape, gradient.dtype),
            pltpu.VMEM(residual.shape, residual.dtype),
            pltpu.SMEM(block_ids.shape, jnp.int32),
            pltpu.SMEM(block_counts.shape, jnp.int32),
            pair((2,)),
            pair((2, EARLY_STEPS)),
            pair((EARLY_STEPS,)),
        ],
    )(block_ids, block_counts, gradient, residual)
    update, left = pl.pallas_call(
        functools.partial(exchange, sections, replicas),
        out_shape=(
            pltpu.VMEM((row_count, col_count), jnp.bfloat16),
            pltpu.VMEM((replicas, block_total, BLK, col_count), jnp.float32),
        ),
        in_specs=[pl.BlockSpec(memory_space=pl.ANY)] * 5,
        out_specs=(pl.BlockSpec(memory_space=pltpu.VMEM),) * 2,
        scratch_shapes=[
            [pltpu.VMEM((block_total, BLK, col_count), jnp.bfloat16)] * replicas,
            [pltpu.VMEM((block_total, BLK, col_count), jnp.float32)] * replicas,
            pltpu.VMEM((replicas, slot_rows, col_count), jnp.bfloat16),
            pltpu.VMEM((1, LANES), jnp.int32),
            pltpu.SMEM(block_ids.shape, jnp.int32),
            pltpu.SMEM(block_counts.shape, jnp.int32),
            pair((2,)),
            pair((2, replicas)),
            pltpu.SemaphoreType.REGULAR,
            pltpu.VMEM((half - 1, over_rows, col_count), jnp.bfloat16),
            pltpu.VMEM((half - 1, 1, LANES), jnp.int32),
            pltpu.VMEM((half - 1, slot_rows, col_count), jnp.bfloat16),
            pltpu.VMEM((half, 1, LANES), jnp.int32),
            pltpu.VMEM((half, cap_rows, col_count), jnp.bfloat16),
            pltpu.VMEM((over_rows, col_count), jnp.bfloat16),
            pltpu.VMEM((over_rows, col_count), jnp.bfloat16),
            pair((2, half - 1)),
            pair((2, half - 1)),
            pair((2, half - 1)),
            pair((2, half)),
            pair((2, half)),
            pair((2, 1)),
            pltpu.VMEM((half // 2 - 1, over_rows, col_count), jnp.bfloat16),
            pltpu.VMEM((over_rows, col_count), jnp.bfloat16),
            pltpu.VMEM((over_rows, col_count), jnp.bfloat16),
            pair((2, half // 2 - 1)),
            pair((2, 1)),
            pltpu.VMEM((1, LANES), jnp.float32),
            pltpu.VMEM((total - 1, 1, LANES), jnp.float32),
            pltpu.SemaphoreType.DMA,
            pltpu.SemaphoreType.DMA,
        ],
        compiler_params=pltpu.CompilerParams(collective_id=0, has_side_effects=True),
    )(
        block_ids,
        block_counts,
        gradient,
        residual,
        early,
    )
    update, left = pl.pallas_call(
        functools.partial(deliver, replicas, starts_early),
        out_shape=(
            jax.ShapeDtypeStruct(update.shape, update.dtype),
            jax.ShapeDtypeStruct((block_total, BLK, width), left.dtype),
        ),
        in_specs=[pl.BlockSpec(memory_space=pl.ANY)] * 2 + [pl.BlockSpec(memory_space=pltpu.HBM)],
        out_specs=(pl.BlockSpec(memory_space=pltpu.HBM),) * 2,
        input_output_aliases={2: 1},
        scratch_shapes=[pltpu.SemaphoreType.DMA((replicas + 1,))],
        compiler_params=pltpu.CompilerParams(vmem_limit_bytes=1 << 20),
    )(update, left, early)
    return (left.reshape(row_count, width), update)


def solution(mesh):
    spec = P("section", "replica")
    sizes = (mesh.shape["section"], mesh.shape["replica"])
    return jax.shard_map(
        functools.partial(per_device, *sizes),
        mesh=mesh,
        in_specs=(spec,) * 4,
        out_specs=(spec, spec),
        check_vma=False,
    )
```

```python
import functools

import jax
import jax.numpy as jnp
from jax import lax
from jax.experimental import pallas as pl
from jax.experimental.pallas import tpu as pltpu
from jax.sharding import PartitionSpec as P

BLK = 8
LANES = 128
EARLY_STEPS = 8
MESH = pl.DeviceIdType.MESH

scale_level = 1.0
epsilon = 1e-06


def flip(index, mask):
    bit, out = 1, index
    while bit <= mask:
        if mask & bit:
            out = out + bit - 2 * bit * (index // bit % 2)
        bit *= 2
    return out


def exchange(
    sections,
    replicas,
    ids_hbm,
    counts_hbm,
    gradient_hbm,
    residual_hbm,
    early_hbm,
    update_ref,
    left_ref,
    grad_buf,
    res_buf,
    packed,
    target_row,
    ids_ref,
    counts_ref,
    list_sems,
    load_sems,
    ready,
    relayed,
    near_rows_buf,
    near_buf,
    far_rows_buf,
    far_buf,
    cross_buf,
    cross_in,
    relay_sems,
    near_row_sems,
    near_sems,
    far_row_sems,
    far_sems,
    cross_sems,
    mate_buf,
    over_buf,
    near_over,
    mate_sems,
    over_sems,
    square_row,
    squares,
    norm_send,
    norm_recv,
):
    block_total, _, width = residual_hbm.shape
    row_count = block_total * BLK
    slot_count = ids_hbm.shape[1]
    slot_rows = slot_count * BLK
    cap = slot_count // 2
    cap_rows = cap * BLK
    half = replicas // 2
    col_count = width // replicas
    section = lax.axis_index("section")
    replica = lax.axis_index("replica")

    def ahead(here, extent):
        return [here] + [
            jnp.where(here + k >= extent, here + k - extent, here + k) for k in range(1, extent)
        ]

    section_at = ahead(section, sections)
    peer_at = [flip(replica, mask) for mask in range(replicas)]
    others = [(i, j) for i in range(sections) for j in range(replicas) if i + j > 0]

    lists = [
        pltpu.make_async_copy(ids_hbm, ids_ref, list_sems.at[0]),
        pltpu.make_async_copy(counts_hbm, counts_ref, list_sems.at[1]),
    ]
    for copy in lists:
        copy.start()

    quarter = replicas // 4
    part_at = replica // quarter
    lower = part_at < 2
    inner = (part_at == 1) | (part_at == 2)
    beside = [half + quarter + low for low in range(quarter)]
    beyond = [half + low for low in range(quarter)]

    def greet(i, j):
        pl.semaphore_signal(
            barrier,
            inc=1,
            device_id={"section": section_at[i], "replica": peer_at[j]},
            device_id_type=MESH,
        )

    barrier = pltpu.get_barrier_semaphore()
    for j in range(1, half):
        greet(0, j)
    for i in range(1, sections):
        greet(i, 0)
    for j in beside:
        pl.when(lower | inner)(functools.partial(greet, 0, j))
    for j in beyond:
        pl.when(lower)(functools.partial(greet, 0, j))
    greeted = half - 1 + sections - 1 + jnp.where(lower, jnp.where(inner, quarter, 0), half)

    order = list(range(replicas - 1, -1, -1))
    same = list(range(1, quarter))
    next_to = list(range(quarter, half))
    loads = {}
    for mask in order:
        cols = pl.ds(pl.multiple_of(peer_at[mask] * col_count, col_count), col_count)
        loads[mask] = (
            pltpu.make_async_copy(gradient_hbm.at[:, :, cols], grad_buf[mask], load_sems.at[0, mask]),
            pltpu.make_async_copy(residual_hbm.at[:, :, cols], res_buf[mask], load_sems.at[1, mask]),
        )
        for copy in loads[mask]:
            copy.start()

    for copy in lists:
        copy.wait()
    count = counts_ref[0, 0]
    ids = [ids_ref[0, s] for s in range(slot_count)]
    lane = lax.broadcasted_iota(jnp.int32, (1, LANES), 1)
    row = jnp.full((1, LANES), -1, jnp.int32)
    for s in range(slot_count):
        base = jnp.where(s < count, ids[s] * BLK, -2 * row_count)
        row = jnp.where(lane // BLK == s, base + lane % BLK, row)
    target_row[...] = row

    def arrive(mask):
        for copy in loads[mask]:
            copy.wait()

    def pack_slots(mask, first, last):
        for s in range(first, last, 2):
            pair = []
            for i in (s, s + 1):
                value = grad_buf[mask][ids[i]].astype(jnp.float32) + res_buf[mask][ids[i]]
                if s >= cap:
                    value = jnp.where(i < count, value, 0.0)
                pair.append(value)
            packed[mask, pl.ds(s * BLK, 2 * BLK), :] = jnp.concatenate(pair, axis=0).astype(jnp.bfloat16)

    def pack(mask):
        arrive(mask)
        pack_slots(mask, 0, slot_count)

    def make(src, dst, sems, slot, peer):
        return pltpu.make_async_remote_copy(
            src_ref=src,
            dst_ref=dst,
            send_sem=sems.at[0, slot],
            recv_sem=sems.at[1, slot],
            device_id={"replica": peer},
            device_id_type=MESH,
        )

    relay_in, near_rows, near, far_rows, far = {}, {}, {}, {}, {}
    for mask in range(1, half):
        peer = peer_at[mask]
        relay_in[mask] = make(
            packed.at[half + mask, pl.ds(cap_rows, slot_rows - cap_rows)],
            relayed.at[mask - 1],
            relay_sems,
            mask - 1,
            peer,
        )
        near_rows[mask] = make(target_row, near_rows_buf.at[mask - 1], near_row_sems, mask - 1, peer)
        rows = pl.ds(0, slot_rows if mask in same else cap_rows)
        near[mask] = make(packed.at[mask, rows], near_buf.at[mask - 1, rows], near_sems, mask - 1, peer)
    for mask in range(half, replicas):
        peer, slot = peer_at[mask], mask - half
        far_rows[mask] = make(target_row, far_rows_buf.at[slot], far_row_sems, slot, peer)
        far[mask] = make(packed.at[mask, pl.ds(0, cap_rows)], far_buf.at[slot], far_sems, slot, peer)
    mate = {}
    for mask in same:
        mate[mask] = make(
            packed.at[quarter + mask, pl.ds(cap_rows, slot_rows - cap_rows)],
            mate_buf.at[mask - 1],
            mate_sems,
            mask - 1,
            peer_at[mask],
        )
    over = make(over_buf, near_over, over_sems, 0, peer_at[quarter])
    cross = make(cross_buf, cross_in, cross_sems, 0, peer_at[half])

    def start_far(masks):
        for mask in masks:
            far_rows[mask].start()
            far[mask].start()

    def tell(mask):
        pl.semaphore_signal(ready, inc=1, device_id={"replica": peer_at[mask]}, device_id_type=MESH)

    def start_near(masks):
        for mask in masks:
            near_rows[mask].start()
            near[mask].start()

    urgent = order[: half - 1]
    for mask in urgent:
        arrive(mask)
        pack_slots(mask, cap, slot_count)
    pl.semaphore_wait(barrier, greeted)
    @pl.when(part_at == 2)
    def _():
        tell(half + quarter)
        tell(half)

    for mask in next_to + same:
        relay_in[mask].start()
    for mask in urgent:
        pack_slots(mask, 0, cap)
    pl.when(inner)(functools.partial(start_far, beside))
    pack(half)
    pl.when(part_at == 2)(functools.partial(start_far, beyond[::-1]))
    for mask in order[half:]:
        if mask not in urgent:
            pack(mask)
    for mask in same:
        mate[mask].start()
    @pl.when(part_at == 3)
    def _():
        start_far(beyond[::-1])
        start_far(beside)

    @pl.when(part_at == 1)
    def _():
        pl.semaphore_wait(ready, 1)
        start_far(beyond[::-1])

    for mask in range(half - 1, 0, -1):
        relay_in[mask].wait_send()

    @pl.when(part_at == 0)
    def _():
        pl.semaphore_wait(ready, 1)
        start_far(beside)
        start_far(beyond[::-1])

    start_near(next_to[::-1] + same)

    for b in range(block_total):
        chosen = jnp.int32(0)
        for s in range(slot_count):
            chosen = jnp.where((ids[s] == b) & (s < count), 1, chosen)
        for mask in order:
            value = grad_buf[mask][b].astype(jnp.float32) + res_buf[mask][b]
            rounded = value.astype(jnp.bfloat16).astype(jnp.float32)
            left_ref[mask, b] = value - jnp.where(chosen > 0, rounded, 0.0)

    def place(wanted, block):
        row_iota = lax.broadcasted_iota(jnp.int32, (row_count, wanted.shape[1]), 0)
        hot = jnp.where(row_iota == wanted, 1.0, 0.0).astype(jnp.bfloat16)
        return jnp.dot(hot, block, preferred_element_type=jnp.float32)

    crossing = packed[half, cap_rows:, :].astype(jnp.float32)
    for mask in range(half - 1, 0, -1):
        relay_in[mask].wait_recv()
        crossing = crossing + relayed[mask - 1].astype(jnp.float32)
    cross_buf[...] = crossing.astype(jnp.bfloat16)
    cross.start()
    beside_over = packed[quarter, cap_rows:, :].astype(jnp.float32)
    for mask in same:
        mate[mask].wait_recv()
        beside_over = beside_over + mate_buf[mask - 1].astype(jnp.float32)
    over_buf[...] = beside_over.astype(jnp.bfloat16)
    over.start()

    summed = place(target_row[:, :slot_rows], packed[0])
    wanted = jnp.full((1, slot_rows), -1, jnp.int32)
    for mask in range(half - 1, 0, -1):
        near_rows[mask].wait_recv()
        near[mask].wait_recv()
        theirs = near_rows_buf[mask - 1][:, :slot_rows]
        if mask in same:
            summed = summed + place(theirs, near_buf[mask - 1])
        else:
            wanted = jnp.maximum(wanted, theirs)
            summed = summed + place(theirs[:, :cap_rows], near_buf[mask - 1, :cap_rows])
    over.wait_recv()
    summed = summed + place(wanted[:, cap_rows:], near_over[...])
    wanted = jnp.full((1, slot_rows), -1, jnp.int32)
    for mask in range(replicas - 1, half - 1, -1):
        far_rows[mask].wait_recv()
        far[mask].wait_recv()
        theirs = far_rows_buf[mask - half][:, :slot_rows]
        wanted = jnp.maximum(wanted, theirs)
        summed = summed + place(theirs[:, :cap_rows], far_buf[mask - half])
    cross.wait_recv()
    summed = summed + place(wanted[:, cap_rows:], cross_in[...])

    lanes = jnp.sum(summed * summed, axis=0, keepdims=True)
    part = lanes[:, :LANES]
    for j in range(1, col_count // LANES):
        part = part + lanes[:, j * LANES : (j + 1) * LANES]
    square_row[...] = part

    for slot, (i, j) in reversed(list(enumerate(others))):
        pltpu.make_async_remote_copy(
            src_ref=square_row,
            dst_ref=squares.at[slot],
            send_sem=norm_send,
            recv_sem=norm_recv,
            device_id={"section": section_at[i], "replica": peer_at[j]},
            device_id_type=MESH,
        ).start()
    for group in (near_rows, near, far_rows, far, mate, {0: cross, 1: over}):
        for copy in group.values():
            copy.wait_send()
    pltpu.make_async_copy(squares, squares, norm_recv).wait()
    pltpu.make_async_copy(squares, squares, norm_send).wait()
    norm_total = jnp.sum(part + jnp.sum(squares[...], axis=0), axis=1, keepdims=True)
    element_count = sections * row_count * width
    root_mean = jnp.sqrt(norm_total / element_count + epsilon)
    clip_factor = scale_level / root_mean
    update_ref[...] = (summed * clip_factor).astype(jnp.bfloat16)


def residual_early(early, ids_hbm, counts_hbm, gradient_hbm, residual_hbm, left_hbm, *scratch):
    grad_buf, res_buf, ids_ref, counts_ref, list_sems, load_sems, out_sems = scratch
    block_total = residual_hbm.shape[0]
    slot_count = ids_hbm.shape[1]
    step = block_total // EARLY_STEPS

    @pl.when(early())
    def _():
        lists = [
            pltpu.make_async_copy(ids_hbm, ids_ref, list_sems.at[0]),
            pltpu.make_async_copy(counts_hbm, counts_ref, list_sems.at[1]),
        ]
        for copy in lists:
            copy.start()
        loads, stores = [], []
        for c in range(EARLY_STEPS):
            part = pl.ds(c * step, step)
            loads.append(
                (
                    pltpu.make_async_copy(gradient_hbm.at[part], grad_buf.at[part], load_sems.at[0, c]),
                    pltpu.make_async_copy(residual_hbm.at[part], res_buf.at[part], load_sems.at[1, c]),
                )
            )
            stores.append(pltpu.make_async_copy(res_buf.at[part], left_hbm.at[part], out_sems.at[c]))
            for copy in loads[c]:
                copy.start()
        for copy in lists:
            copy.wait()
        for c in range(EARLY_STEPS):
            for copy in loads[c]:
                copy.wait()
            for b in range(c * step, (c + 1) * step):
                chosen = jnp.int32(0)
                for s in range(slot_count):
                    chosen = jnp.where((ids_ref[0, s] == b) & (s < counts_ref[0, 0]), 1, chosen)
                value = grad_buf[b].astype(jnp.float32) + res_buf[b]
                rounded = value.astype(jnp.bfloat16).astype(jnp.float32)
                res_buf[b] = value - jnp.where(chosen > 0, rounded, 0.0)
            stores[c].start()
        for copy in stores:
            copy.wait()


def starts_early():
    return (lax.axis_index("replica") == 0) & (lax.axis_index("section") < 2)


def deliver(replicas, early, update_ref, left_ref, early_hbm, update_hbm, left_hbm, sems):
    col_count = left_ref.shape[3]
    replica = lax.axis_index("replica")
    update_copy = pltpu.make_async_copy(update_ref, update_hbm, sems.at[replicas])
    update_copy.start()

    @pl.when(jnp.logical_not(early()))
    def _():
        copies = []
        for mask in range(replicas):
            cols = pl.ds(pl.multiple_of(flip(replica, mask) * col_count, col_count), col_count)
            copies.append(pltpu.make_async_copy(left_ref.at[mask], left_hbm.at[:, :, cols], sems.at[mask]))
        for copy in copies:
            copy.start()
        for copy in copies:
            copy.wait()

    update_copy.wait()


def per_device(sections, replicas, gradient, residual, block_ids, block_counts):
    row_count, width = gradient.shape
    block_total = row_count // BLK
    slot_count = block_ids.shape[1]
    col_count = width // replicas
    total = sections * replicas
    slot_rows = slot_count * BLK
    cap_rows = slot_count // 2 * BLK
    over_rows = slot_rows - cap_rows
    half = replicas // 2
    pair = pltpu.SemaphoreType.DMA
    gradient = gradient.reshape(block_total, BLK, width)
    residual = residual.reshape(block_total, BLK, width)
    early = pl.pallas_call(
        functools.partial(residual_early, starts_early),
        out_shape=jax.ShapeDtypeStruct(residual.shape, residual.dtype),
        in_specs=[pl.BlockSpec(memory_space=pl.ANY)] * 4,
        out_specs=pl.BlockSpec(memory_space=pltpu.HBM),
        scratch_shapes=[
            pltpu.VMEM(gradient.shape, gradient.dtype),
            pltpu.VMEM(residual.shape, residual.dtype),
            pltpu.SMEM(block_ids.shape, jnp.int32),
            pltpu.SMEM(block_counts.shape, jnp.int32),
            pair((2,)),
            pair((2, EARLY_STEPS)),
            pair((EARLY_STEPS,)),
        ],
    )(block_ids, block_counts, gradient, residual)
    update, left = pl.pallas_call(
        functools.partial(exchange, sections, replicas),
        out_shape=(
            pltpu.VMEM((row_count, col_count), jnp.bfloat16),
            pltpu.VMEM((replicas, block_total, BLK, col_count), jnp.float32),
        ),
        in_specs=[pl.BlockSpec(memory_space=pl.ANY)] * 5,
        out_specs=(pl.BlockSpec(memory_space=pltpu.VMEM),) * 2,
        scratch_shapes=[
            [pltpu.VMEM((block_total, BLK, col_count), jnp.bfloat16)] * replicas,
            [pltpu.VMEM((block_total, BLK, col_count), jnp.float32)] * replicas,
            pltpu.VMEM((replicas, slot_rows, col_count), jnp.bfloat16),
            pltpu.VMEM((1, LANES), jnp.int32),
            pltpu.SMEM(block_ids.shape, jnp.int32),
            pltpu.SMEM(block_counts.shape, jnp.int32),
            pair((2,)),
            pair((2, replicas)),
            pltpu.SemaphoreType.REGULAR,
            pltpu.VMEM((half - 1, over_rows, col_count), jnp.bfloat16),
            pltpu.VMEM((half - 1, 1, LANES), jnp.int32),
            pltpu.VMEM((half - 1, slot_rows, col_count), jnp.bfloat16),
            pltpu.VMEM((half, 1, LANES), jnp.int32),
            pltpu.VMEM((half, cap_rows, col_count), jnp.bfloat16),
            pltpu.VMEM((over_rows, col_count), jnp.bfloat16),
            pltpu.VMEM((over_rows, col_count), jnp.bfloat16),
            pair((2, half - 1)),
            pair((2, half - 1)),
            pair((2, half - 1)),
            pair((2, half)),
            pair((2, half)),
            pair((2, 1)),
            pltpu.VMEM((half // 2 - 1, over_rows, col_count), jnp.bfloat16),
            pltpu.VMEM((over_rows, col_count), jnp.bfloat16),
            pltpu.VMEM((over_rows, col_count), jnp.bfloat16),
            pair((2, half // 2 - 1)),
            pair((2, 1)),
            pltpu.VMEM((1, LANES), jnp.float32),
            pltpu.VMEM((total - 1, 1, LANES), jnp.float32),
            pltpu.SemaphoreType.DMA,
            pltpu.SemaphoreType.DMA,
        ],
        compiler_params=pltpu.CompilerParams(collective_id=0, has_side_effects=True),
    )(
        block_ids,
        block_counts,
        gradient,
        residual,
        early,
    )
    update, left = pl.pallas_call(
        functools.partial(deliver, replicas, starts_early),
        out_shape=(
            jax.ShapeDtypeStruct(update.shape, update.dtype),
            jax.ShapeDtypeStruct((block_total, BLK, width), left.dtype),
        ),
        in_specs=[pl.BlockSpec(memory_space=pl.ANY)] * 2 + [pl.BlockSpec(memory_space=pltpu.HBM)],
        out_specs=(pl.BlockSpec(memory_space=pltpu.HBM),) * 2,
        input_output_aliases={2: 1},
        scratch_shapes=[pltpu.SemaphoreType.DMA((replicas + 1,))],
        compiler_params=pltpu.CompilerParams(vmem_limit_bytes=1 << 20),
    )(update, left, early)
    return (left.reshape(row_count, width), update)


def solution(mesh):
    spec = P("section", "replica")
    sizes = (mesh.shape["section"], mesh.shape["replica"])
    return jax.shard_map(
        functools.partial(per_device, *sizes),
        mesh=mesh,
        in_specs=(spec,) * 4,
        out_specs=(spec, spec),
        check_vma=False,
    )
```

```python
import functools

import jax
import jax.numpy as jnp
from jax import lax
from jax.experimental import pallas as pl
from jax.experimental.pallas import tpu as pltpu
from jax.sharding import PartitionSpec as P

BLK = 8
LANES = 128
EARLY_STEPS = 8
MESH = pl.DeviceIdType.MESH

scale_level = 1.0
epsilon = 1e-06


def flip(index, mask):
    bit, out = 1, index
    while bit <= mask:
        if mask & bit:
            out = out + bit - 2 * bit * (index // bit % 2)
        bit *= 2
    return out


def exchange(
    sections,
    replicas,
    ids_hbm,
    counts_hbm,
    gradient_hbm,
    residual_hbm,
    early_hbm,
    update_ref,
    left_ref,
    grad_buf,
    res_buf,
    packed,
    target_row,
    ids_ref,
    counts_ref,
    list_sems,
    load_sems,
    ready,
    relayed,
    near_rows_buf,
    near_buf,
    far_rows_buf,
    far_buf,
    cross_buf,
    cross_in,
    relay_sems,
    near_row_sems,
    near_sems,
    far_row_sems,
    far_sems,
    cross_sems,
    mate_buf,
    over_buf,
    near_over,
    mate_sems,
    over_sems,
    square_row,
    squares,
    norm_send,
    norm_recv,
):
    block_total, _, width = residual_hbm.shape
    row_count = block_total * BLK
    slot_count = ids_hbm.shape[1]
    slot_rows = slot_count * BLK
    cap = slot_count // 2
    cap_rows = cap * BLK
    half = replicas // 2
    col_count = width // replicas
    section = lax.axis_index("section")
    replica = lax.axis_index("replica")

    def ahead(here, extent):
        return [here] + [
            jnp.where(here + k >= extent, here + k - extent, here + k) for k in range(1, extent)
        ]

    section_at = ahead(section, sections)
    peer_at = [flip(replica, mask) for mask in range(replicas)]
    others = [(i, j) for i in range(sections) for j in range(replicas) if i + j > 0]

    lists = [
        pltpu.make_async_copy(ids_hbm, ids_ref, list_sems.at[0]),
        pltpu.make_async_copy(counts_hbm, counts_ref, list_sems.at[1]),
    ]
    for copy in lists:
        copy.start()

    quarter = replicas // 4
    part_at = replica // quarter
    lower = part_at < 2
    inner = (part_at == 1) | (part_at == 2)
    beside = [half + quarter + low for low in range(quarter)]
    beyond = [half + low for low in range(quarter)]

    def greet(i, j):
        pl.semaphore_signal(
            barrier,
            inc=1,
            device_id={"section": section_at[i], "replica": peer_at[j]},
            device_id_type=MESH,
        )

    barrier = pltpu.get_barrier_semaphore()
    for j in range(1, half):
        greet(0, j)
    for i in range(1, sections):
        greet(i, 0)
    for j in beside:
        pl.when(lower | inner)(functools.partial(greet, 0, j))
    for j in beyond:
        pl.when(lower)(functools.partial(greet, 0, j))
    greeted = half - 1 + sections - 1 + jnp.where(lower, jnp.where(inner, quarter, 0), half)

    order = list(range(replicas - 1, -1, -1))
    same = list(range(1, quarter))
    next_to = list(range(quarter, half))
    loads = {}
    for mask in order:
        cols = pl.ds(pl.multiple_of(peer_at[mask] * col_count, col_count), col_count)
        loads[mask] = (
            pltpu.make_async_copy(gradient_hbm.at[:, :, cols], grad_buf[mask], load_sems.at[0, mask]),
            pltpu.make_async_copy(residual_hbm.at[:, :, cols], res_buf[mask], load_sems.at[1, mask]),
        )
        for copy in loads[mask]:
            copy.start()

    for copy in lists:
        copy.wait()
    count = counts_ref[0, 0]
    ids = [ids_ref[0, s] for s in range(slot_count)]
    lane = lax.broadcasted_iota(jnp.int32, (1, LANES), 1)
    row = jnp.full((1, LANES), -1, jnp.int32)
    for s in range(slot_count):
        base = jnp.where(s < count, ids[s] * BLK, -2 * row_count)
        row = jnp.where(lane // BLK == s, base + lane % BLK, row)
    target_row[...] = row

    def arrive(mask):
        for copy in loads[mask]:
            copy.wait()

    def pack_slots(mask, first, last):
        for s in range(first, last, 2):
            pair = []
            for i in (s, s + 1):
                value = grad_buf[mask][ids[i]].astype(jnp.float32) + res_buf[mask][ids[i]]
                if s >= cap:
                    value = jnp.where(i < count, value, 0.0)
                pair.append(value)
            packed[mask, pl.ds(s * BLK, 2 * BLK), :] = jnp.concatenate(pair, axis=0).astype(jnp.bfloat16)

    def pack(mask):
        arrive(mask)
        pack_slots(mask, 0, slot_count)

    def make(src, dst, sems, slot, peer):
        return pltpu.make_async_remote_copy(
            src_ref=src,
            dst_ref=dst,
            send_sem=sems.at[0, slot],
            recv_sem=sems.at[1, slot],
            device_id={"replica": peer},
            device_id_type=MESH,
        )

    relay_in, near_rows, near, far_rows, far = {}, {}, {}, {}, {}
    for mask in range(1, half):
        peer = peer_at[mask]
        relay_in[mask] = make(
            packed.at[half + mask, pl.ds(cap_rows, slot_rows - cap_rows)],
            relayed.at[mask - 1],
            relay_sems,
            mask - 1,
            peer,
        )
        near_rows[mask] = make(target_row, near_rows_buf.at[mask - 1], near_row_sems, mask - 1, peer)
        rows = pl.ds(0, slot_rows if mask in same else cap_rows)
        near[mask] = make(packed.at[mask, rows], near_buf.at[mask - 1, rows], near_sems, mask - 1, peer)
    for mask in range(half, replicas):
        peer, slot = peer_at[mask], mask - half
        far_rows[mask] = make(target_row, far_rows_buf.at[slot], far_row_sems, slot, peer)
        far[mask] = make(packed.at[mask, pl.ds(0, cap_rows)], far_buf.at[slot], far_sems, slot, peer)
    mate = {}
    for mask in same:
        mate[mask] = make(
            packed.at[quarter + mask, pl.ds(cap_rows, slot_rows - cap_rows)],
            mate_buf.at[mask - 1],
            mate_sems,
            mask - 1,
            peer_at[mask],
        )
    over = make(over_buf, near_over, over_sems, 0, peer_at[quarter])
    cross = make(cross_buf, cross_in, cross_sems, 0, peer_at[half])

    def start_far(masks):
        for mask in masks:
            far_rows[mask].start()
            far[mask].start()

    def tell(mask):
        pl.semaphore_signal(ready, inc=1, device_id={"replica": peer_at[mask]}, device_id_type=MESH)

    def start_near(masks):
        for mask in masks:
            near_rows[mask].start()
            near[mask].start()

    urgent = order[: half - 1]
    for mask in urgent:
        arrive(mask)
        pack_slots(mask, cap, slot_count)
    pl.semaphore_wait(barrier, greeted)
    @pl.when(part_at == 2)
    def _():
        tell(half + quarter)
        tell(half)

    for mask in next_to[::-1] + same:
        relay_in[mask].start()
    for mask in urgent:
        pack_slots(mask, 0, cap)
    pl.when(inner)(functools.partial(start_far, beside))
    pack(half)
    pl.when(part_at == 2)(functools.partial(start_far, beyond[::-1]))
    for mask in order[half:]:
        if mask not in urgent:
            pack(mask)
    for mask in same:
        mate[mask].start()
    @pl.when(part_at == 3)
    def _():
        start_far(beyond[::-1])
        start_far(beside)

    @pl.when(part_at == 1)
    def _():
        pl.semaphore_wait(ready, 1)
        start_far(beyond[::-1])

    for mask in range(half - 1, 0, -1):
        relay_in[mask].wait_send()

    @pl.when(part_at == 0)
    def _():
        pl.semaphore_wait(ready, 1)
        start_far(beside)
        start_far(beyond[::-1])

    start_near(next_to[::-1] + same)

    for b in range(block_total):
        chosen = jnp.int32(0)
        for s in range(slot_count):
            chosen = jnp.where((ids[s] == b) & (s < count), 1, chosen)
        for mask in order:
            value = grad_buf[mask][b].astype(jnp.float32) + res_buf[mask][b]
            rounded = value.astype(jnp.bfloat16).astype(jnp.float32)
            left_ref[mask, b] = value - jnp.where(chosen > 0, rounded, 0.0)

    def place(wanted, block):
        row_iota = lax.broadcasted_iota(jnp.int32, (row_count, wanted.shape[1]), 0)
        hot = jnp.where(row_iota == wanted, 1.0, 0.0).astype(jnp.bfloat16)
        return jnp.dot(hot, block, preferred_element_type=jnp.float32)

    crossing = packed[half, cap_rows:, :].astype(jnp.float32)
    for mask in range(half - 1, 0, -1):
        relay_in[mask].wait_recv()
        crossing = crossing + relayed[mask - 1].astype(jnp.float32)
    cross_buf[...] = crossing.astype(jnp.bfloat16)
    cross.start()
    beside_over = packed[quarter, cap_rows:, :].astype(jnp.float32)
    for mask in same:
        mate[mask].wait_recv()
        beside_over = beside_over + mate_buf[mask - 1].astype(jnp.float32)
    over_buf[...] = beside_over.astype(jnp.bfloat16)
    over.start()

    summed = place(target_row[:, :slot_rows], packed[0])
    wanted = jnp.full((1, slot_rows), -1, jnp.int32)
    for mask in range(half - 1, 0, -1):
        near_rows[mask].wait_recv()
        near[mask].wait_recv()
        theirs = near_rows_buf[mask - 1][:, :slot_rows]
        if mask in same:
            summed = summed + place(theirs, near_buf[mask - 1])
        else:
            wanted = jnp.maximum(wanted, theirs)
            summed = summed + place(theirs[:, :cap_rows], near_buf[mask - 1, :cap_rows])
    far_wanted = jnp.full((1, slot_rows), -1, jnp.int32)
    for mask in range(replicas - 1, half - 1, -1):
        far_rows[mask].wait_recv()
        far[mask].wait_recv()
        theirs = far_rows_buf[mask - half][:, :slot_rows]
        far_wanted = jnp.maximum(far_wanted, theirs)
        summed = summed + place(theirs[:, :cap_rows], far_buf[mask - half])
    over.wait_recv()
    summed = summed + place(wanted[:, cap_rows:], near_over[...])
    cross.wait_recv()
    summed = summed + place(far_wanted[:, cap_rows:], cross_in[...])

    lanes = jnp.sum(summed * summed, axis=0, keepdims=True)
    part = lanes[:, :LANES]
    for j in range(1, col_count // LANES):
        part = part + lanes[:, j * LANES : (j + 1) * LANES]
    square_row[...] = part

    far_first = sorted(
        enumerate(others),
        key=lambda entry: (entry[1][0] * 2 // sections, entry[1][0] % 2 == 0, entry[1][1]),
        reverse=True,
    )
    for slot, (i, j) in far_first:
        pltpu.make_async_remote_copy(
            src_ref=square_row,
            dst_ref=squares.at[slot],
            send_sem=norm_send,
            recv_sem=norm_recv,
            device_id={"section": section_at[i], "replica": peer_at[j]},
            device_id_type=MESH,
        ).start()
    for group in (near_rows, near, far_rows, far, mate, {0: cross, 1: over}):
        for copy in group.values():
            copy.wait_send()
    pltpu.make_async_copy(squares, squares, norm_recv).wait()
    pltpu.make_async_copy(squares, squares, norm_send).wait()
    norm_total = jnp.sum(part + jnp.sum(squares[...], axis=0), axis=1, keepdims=True)
    element_count = sections * row_count * width
    root_mean = jnp.sqrt(norm_total / element_count + epsilon)
    clip_factor = scale_level / root_mean
    update_ref[...] = (summed * clip_factor).astype(jnp.bfloat16)


def residual_early(early, ids_hbm, counts_hbm, gradient_hbm, residual_hbm, left_hbm, *scratch):
    grad_buf, res_buf, ids_ref, counts_ref, list_sems, load_sems, out_sems = scratch
    block_total = residual_hbm.shape[0]
    slot_count = ids_hbm.shape[1]
    step = block_total // EARLY_STEPS

    @pl.when(early())
    def _():
        lists = [
            pltpu.make_async_copy(ids_hbm, ids_ref, list_sems.at[0]),
            pltpu.make_async_copy(counts_hbm, counts_ref, list_sems.at[1]),
        ]
        for copy in lists:
            copy.start()
        loads, stores = [], []
        for c in range(EARLY_STEPS):
            part = pl.ds(c * step, step)
            loads.append(
                (
                    pltpu.make_async_copy(gradient_hbm.at[part], grad_buf.at[part], load_sems.at[0, c]),
                    pltpu.make_async_copy(residual_hbm.at[part], res_buf.at[part], load_sems.at[1, c]),
                )
            )
            stores.append(pltpu.make_async_copy(res_buf.at[part], left_hbm.at[part], out_sems.at[c]))
            for copy in loads[c]:
                copy.start()
        for copy in lists:
            copy.wait()
        for c in range(EARLY_STEPS):
            for copy in loads[c]:
                copy.wait()
            for b in range(c * step, (c + 1) * step):
                chosen = jnp.int32(0)
                for s in range(slot_count):
                    chosen = jnp.where((ids_ref[0, s] == b) & (s < counts_ref[0, 0]), 1, chosen)
                value = grad_buf[b].astype(jnp.float32) + res_buf[b]
                rounded = value.astype(jnp.bfloat16).astype(jnp.float32)
                res_buf[b] = value - jnp.where(chosen > 0, rounded, 0.0)
            stores[c].start()
        for copy in stores:
            copy.wait()


def starts_early():
    return (lax.axis_index("replica") == 0) & (lax.axis_index("section") < 2)


def deliver(replicas, early, update_ref, left_ref, early_hbm, update_hbm, left_hbm, sems):
    col_count = left_ref.shape[3]
    replica = lax.axis_index("replica")
    update_copy = pltpu.make_async_copy(update_ref, update_hbm, sems.at[replicas])
    update_copy.start()

    @pl.when(jnp.logical_not(early()))
    def _():
        copies = []
        for mask in range(replicas):
            cols = pl.ds(pl.multiple_of(flip(replica, mask) * col_count, col_count), col_count)
            copies.append(pltpu.make_async_copy(left_ref.at[mask], left_hbm.at[:, :, cols], sems.at[mask]))
        for copy in copies:
            copy.start()
        for copy in copies:
            copy.wait()

    update_copy.wait()


def per_device(sections, replicas, gradient, residual, block_ids, block_counts):
    row_count, width = gradient.shape
    block_total = row_count // BLK
    slot_count = block_ids.shape[1]
    col_count = width // replicas
    total = sections * replicas
    slot_rows = slot_count * BLK
    cap_rows = slot_count // 2 * BLK
    over_rows = slot_rows - cap_rows
    half = replicas // 2
    pair = pltpu.SemaphoreType.DMA
    gradient = gradient.reshape(block_total, BLK, width)
    residual = residual.reshape(block_total, BLK, width)
    early = pl.pallas_call(
        functools.partial(residual_early, starts_early),
        out_shape=jax.ShapeDtypeStruct(residual.shape, residual.dtype),
        in_specs=[pl.BlockSpec(memory_space=pl.ANY)] * 4,
        out_specs=pl.BlockSpec(memory_space=pltpu.HBM),
        scratch_shapes=[
            pltpu.VMEM(gradient.shape, gradient.dtype),
            pltpu.VMEM(residual.shape, residual.dtype),
            pltpu.SMEM(block_ids.shape, jnp.int32),
            pltpu.SMEM(block_counts.shape, jnp.int32),
            pair((2,)),
            pair((2, EARLY_STEPS)),
            pair((EARLY_STEPS,)),
        ],
    )(block_ids, block_counts, gradient, residual)
    update, left = pl.pallas_call(
        functools.partial(exchange, sections, replicas),
        out_shape=(
            pltpu.VMEM((row_count, col_count), jnp.bfloat16),
            pltpu.VMEM((replicas, block_total, BLK, col_count), jnp.float32),
        ),
        in_specs=[pl.BlockSpec(memory_space=pl.ANY)] * 5,
        out_specs=(pl.BlockSpec(memory_space=pltpu.VMEM),) * 2,
        scratch_shapes=[
            [pltpu.VMEM((block_total, BLK, col_count), jnp.bfloat16)] * replicas,
            [pltpu.VMEM((block_total, BLK, col_count), jnp.float32)] * replicas,
            pltpu.VMEM((replicas, slot_rows, col_count), jnp.bfloat16),
            pltpu.VMEM((1, LANES), jnp.int32),
            pltpu.SMEM(block_ids.shape, jnp.int32),
            pltpu.SMEM(block_counts.shape, jnp.int32),
            pair((2,)),
            pair((2, replicas)),
            pltpu.SemaphoreType.REGULAR,
            pltpu.VMEM((half - 1, over_rows, col_count), jnp.bfloat16),
            pltpu.VMEM((half - 1, 1, LANES), jnp.int32),
            pltpu.VMEM((half - 1, slot_rows, col_count), jnp.bfloat16),
            pltpu.VMEM((half, 1, LANES), jnp.int32),
            pltpu.VMEM((half, cap_rows, col_count), jnp.bfloat16),
            pltpu.VMEM((over_rows, col_count), jnp.bfloat16),
            pltpu.VMEM((over_rows, col_count), jnp.bfloat16),
            pair((2, half - 1)),
            pair((2, half - 1)),
            pair((2, half - 1)),
            pair((2, half)),
            pair((2, half)),
            pair((2, 1)),
            pltpu.VMEM((half // 2 - 1, over_rows, col_count), jnp.bfloat16),
            pltpu.VMEM((over_rows, col_count), jnp.bfloat16),
            pltpu.VMEM((over_rows, col_count), jnp.bfloat16),
            pair((2, half // 2 - 1)),
            pair((2, 1)),
            pltpu.VMEM((1, LANES), jnp.float32),
            pltpu.VMEM((total - 1, 1, LANES), jnp.float32),
            pltpu.SemaphoreType.DMA,
            pltpu.SemaphoreType.DMA,
        ],
        compiler_params=pltpu.CompilerParams(collective_id=0, has_side_effects=True),
    )(
        block_ids,
        block_counts,
        gradient,
        residual,
        early,
    )
    update, left = pl.pallas_call(
        functools.partial(deliver, replicas, starts_early),
        out_shape=(
            jax.ShapeDtypeStruct(update.shape, update.dtype),
            jax.ShapeDtypeStruct((block_total, BLK, width), left.dtype),
        ),
        in_specs=[pl.BlockSpec(memory_space=pl.ANY)] * 2 + [pl.BlockSpec(memory_space=pltpu.HBM)],
        out_specs=(pl.BlockSpec(memory_space=pltpu.HBM),) * 2,
        input_output_aliases={2: 1},
        scratch_shapes=[pltpu.SemaphoreType.DMA((replicas + 1,))],
        compiler_params=pltpu.CompilerParams(vmem_limit_bytes=1 << 20),
    )(update, left, early)
    return (left.reshape(row_count, width), update)


def solution(mesh):
    spec = P("section", "replica")
    sizes = (mesh.shape["section"], mesh.shape["replica"])
    return jax.shard_map(
        functools.partial(per_device, *sizes),
        mesh=mesh,
        in_specs=(spec,) * 4,
        out_specs=(spec, spec),
        check_vma=False,
    )
```

```python
import functools

import jax
import jax.numpy as jnp
from jax import lax
from jax.experimental import pallas as pl
from jax.experimental.pallas import tpu as pltpu
from jax.sharding import PartitionSpec as P

BLK = 8
LANES = 128
EARLY_STEPS = 2
MESH = pl.DeviceIdType.MESH

scale_level = 1.0
epsilon = 1e-06


def flip(index, mask):
    bit, out = 1, index
    while bit <= mask:
        if mask & bit:
            out = out + bit - 2 * bit * (index // bit % 2)
        bit *= 2
    return out


def exchange(
    sections,
    replicas,
    ids_hbm,
    counts_hbm,
    gradient_hbm,
    residual_hbm,
    early_hbm,
    update_ref,
    left_ref,
    grad_buf,
    res_buf,
    packed,
    target_row,
    ids_ref,
    counts_ref,
    list_sems,
    load_sems,
    ready,
    relayed,
    rows_buf,
    near_buf,
    far_buf,
    cross_buf,
    cross_in,
    relay_sems,
    row_sems,
    near_sems,
    far_sems,
    cross_sems,
    mate_buf,
    over_buf,
    near_over,
    mate_sems,
    over_sems,
    square_row,
    squares,
    norm_send,
    norm_recv,
):
    block_total, _, width = residual_hbm.shape
    row_count = block_total * BLK
    slot_count = ids_hbm.shape[1]
    slot_rows = slot_count * BLK
    cap = slot_count // 2
    cap_rows = cap * BLK
    half = replicas // 2
    col_count = width // replicas
    section = lax.axis_index("section")
    replica = lax.axis_index("replica")

    def ahead(here, extent):
        return [here] + [
            jnp.where(here + k >= extent, here + k - extent, here + k) for k in range(1, extent)
        ]

    section_at = ahead(section, sections)
    peer_at = [flip(replica, mask) for mask in range(replicas)]
    others = [(i, j) for i in range(sections) for j in range(replicas) if i + j > 0]

    lists = [
        pltpu.make_async_copy(ids_hbm, ids_ref, list_sems.at[0]),
        pltpu.make_async_copy(counts_hbm, counts_ref, list_sems.at[1]),
    ]
    for copy in lists:
        copy.start()

    quarter = replicas // 4
    part_at = replica // quarter
    lower = part_at < 2
    inner = (part_at == 1) | (part_at == 2)
    beside = [half + quarter + low for low in range(quarter)]
    beyond = [half + low for low in range(quarter)]

    def greet(i, j):
        pl.semaphore_signal(
            barrier,
            inc=1,
            device_id={"section": section_at[i], "replica": peer_at[j]},
            device_id_type=MESH,
        )

    barrier = pltpu.get_barrier_semaphore()
    for j in range(1, half):
        greet(0, j)
    for i in range(1, sections):
        greet(i, 0)
    for j in beside:
        pl.when(lower | inner)(functools.partial(greet, 0, j))
    for j in beyond:
        pl.when(lower)(functools.partial(greet, 0, j))
    greeted = half - 1 + sections - 1 + jnp.where(lower, jnp.where(inner, quarter, 0), half)

    order = list(range(replicas - 1, -1, -1))
    same = list(range(1, quarter))
    next_to = list(range(quarter, half))
    loads = {}
    for mask in order:
        cols = pl.ds(pl.multiple_of(peer_at[mask] * col_count, col_count), col_count)
        loads[mask] = (
            pltpu.make_async_copy(gradient_hbm.at[:, :, cols], grad_buf[mask], load_sems.at[0, mask]),
            pltpu.make_async_copy(residual_hbm.at[:, :, cols], res_buf[mask], load_sems.at[1, mask]),
        )
        for copy in loads[mask]:
            copy.start()

    for copy in lists:
        copy.wait()
    count = counts_ref[0, 0]
    ids = [ids_ref[0, s] for s in range(slot_count)]
    lane = lax.broadcasted_iota(jnp.int32, (1, LANES), 1)
    row = jnp.full((1, LANES), -1, jnp.int32)
    for s in range(slot_count):
        base = jnp.where(s < count, ids[s] * BLK, -2 * row_count)
        row = jnp.where(lane // BLK == s, base + lane % BLK, row)
    target_row[...] = row

    def arrive(mask):
        for copy in loads[mask]:
            copy.wait()

    def pack_slots(mask, first, last):
        for s in range(first, last, 2):
            pair = []
            for i in (s, s + 1):
                value = grad_buf[mask][ids[i]].astype(jnp.float32) + res_buf[mask][ids[i]]
                if s >= cap:
                    value = jnp.where(i < count, value, 0.0)
                pair.append(value)
            packed[mask, pl.ds(s * BLK, 2 * BLK), :] = jnp.concatenate(pair, axis=0).astype(jnp.bfloat16)

    def pack(mask):
        arrive(mask)
        pack_slots(mask, 0, slot_count)

    def make(src, dst, sems, slot, peer):
        return pltpu.make_async_remote_copy(
            src_ref=src,
            dst_ref=dst,
            send_sem=sems.at[0, slot],
            recv_sem=sems.at[1, slot],
            device_id={"replica": peer},
            device_id_type=MESH,
        )

    relay_in, near_rows, near, far_rows, far = {}, {}, {}, {}, {}
    for mask in range(1, half):
        peer = peer_at[mask]
        relay_in[mask] = make(
            packed.at[half + mask, pl.ds(cap_rows, slot_rows - cap_rows)],
            relayed.at[mask - 1],
            relay_sems,
            mask - 1,
            peer,
        )
        near_rows[mask] = make(target_row, rows_buf.at[mask - 1], row_sems, 0, peer)
        rows = pl.ds(0, slot_rows if mask in same else cap_rows)
        near[mask] = make(packed.at[mask, rows], near_buf.at[mask - 1, rows], near_sems, mask - 1, peer)
    for mask in range(half, replicas):
        peer, slot = peer_at[mask], mask - half
        far_rows[mask] = make(target_row, rows_buf.at[mask - 1], row_sems, 0, peer)
        far[mask] = make(packed.at[mask, pl.ds(0, cap_rows)], far_buf.at[slot], far_sems, slot, peer)
    mate = {}
    for mask in same:
        mate[mask] = make(
            packed.at[quarter + mask, pl.ds(cap_rows, slot_rows - cap_rows)],
            mate_buf.at[mask - 1],
            mate_sems,
            mask - 1,
            peer_at[mask],
        )
    over = make(over_buf, near_over, over_sems, 0, peer_at[quarter])
    cross = make(cross_buf, cross_in, cross_sems, 0, peer_at[half])

    def start_far(masks):
        for mask in masks:
            far_rows[mask].start()
            far[mask].start()

    def tell(mask):
        pl.semaphore_signal(ready, inc=1, device_id={"replica": peer_at[mask]}, device_id_type=MESH)

    def start_near(masks):
        for mask in masks:
            near_rows[mask].start()
            near[mask].start()

    urgent = order[: half - 1]
    for mask in urgent:
        arrive(mask)
        pack_slots(mask, cap, slot_count)
    pl.semaphore_wait(barrier, greeted)
    @pl.when(part_at == 2)
    def _():
        tell(half + quarter)
        tell(half)

    for mask in next_to[::-1] + same:
        relay_in[mask].start()
    for mask in urgent:
        pack_slots(mask, 0, cap)
    pl.when(inner)(functools.partial(start_far, beside))
    pack(half)
    pl.when(part_at == 2)(functools.partial(start_far, beyond[::-1]))
    for mask in order[half:]:
        if mask not in urgent:
            pack(mask)
    for mask in same:
        mate[mask].start()
    @pl.when(part_at == 3)
    def _():
        start_far(beyond[::-1])
        start_far(beside)

    @pl.when(part_at == 1)
    def _():
        pl.semaphore_wait(ready, 1)
        start_far(beyond[::-1])

    for mask in range(half - 1, 0, -1):
        relay_in[mask].wait_send()

    @pl.when(part_at == 0)
    def _():
        pl.semaphore_wait(ready, 1)
        start_far(beside)
        start_far(beyond[::-1])

    start_near(next_to[::-1] + same)

    for b in range(block_total):
        chosen = jnp.int32(0)
        for s in range(slot_count):
            chosen = jnp.where((ids[s] == b) & (s < count), 1, chosen)
        for mask in order:
            value = grad_buf[mask][b].astype(jnp.float32) + res_buf[mask][b]
            rounded = value.astype(jnp.bfloat16).astype(jnp.float32)
            left_ref[mask, b] = value - jnp.where(chosen > 0, rounded, 0.0)

    def place(wanted, block):
        row_iota = lax.broadcasted_iota(jnp.int32, (row_count, wanted.shape[1]), 0)
        hot = jnp.where(row_iota == wanted, 1.0, 0.0).astype(jnp.bfloat16)
        return jnp.dot(hot, block, preferred_element_type=jnp.float32)

    crossing = packed[half, cap_rows:, :].astype(jnp.float32)
    for mask in range(half - 1, 0, -1):
        relay_in[mask].wait_recv()
        crossing = crossing + relayed[mask - 1].astype(jnp.float32)
    cross_buf[...] = crossing.astype(jnp.bfloat16)
    cross.start()
    beside_over = packed[quarter, cap_rows:, :].astype(jnp.float32)
    for mask in same:
        mate[mask].wait_recv()
        beside_over = beside_over + mate_buf[mask - 1].astype(jnp.float32)
    over_buf[...] = beside_over.astype(jnp.bfloat16)
    over.start()

    summed = place(target_row[:, :slot_rows], packed[0])
    pltpu.make_async_copy(rows_buf, rows_buf, row_sems.at[1, 0]).wait()
    wanted = jnp.full((1, slot_rows), -1, jnp.int32)
    for mask in range(half - 1, 0, -1):
        near[mask].wait_recv()
        theirs = rows_buf[mask - 1][:, :slot_rows]
        if mask in same:
            summed = summed + place(theirs, near_buf[mask - 1])
        else:
            wanted = jnp.maximum(wanted, theirs)
            summed = summed + place(theirs[:, :cap_rows], near_buf[mask - 1, :cap_rows])
    far_wanted = jnp.full((1, slot_rows), -1, jnp.int32)
    for mask in range(replicas - 1, half - 1, -1):
        far[mask].wait_recv()
        theirs = rows_buf[mask - 1][:, :slot_rows]
        far_wanted = jnp.maximum(far_wanted, theirs)
        summed = summed + place(theirs[:, :cap_rows], far_buf[mask - half])
    over.wait_recv()
    summed = summed + place(wanted[:, cap_rows:], near_over[...])
    cross.wait_recv()
    summed = summed + place(far_wanted[:, cap_rows:], cross_in[...])

    lanes = jnp.sum(summed * summed, axis=0, keepdims=True)
    part = lanes[:, :LANES]
    for j in range(1, col_count // LANES):
        part = part + lanes[:, j * LANES : (j + 1) * LANES]
    square_row[...] = part

    far_first = sorted(
        enumerate(others),
        key=lambda entry: (entry[1][0] * 2 // sections, entry[1][0] % 2 == 0, entry[1][1]),
        reverse=True,
    )
    for slot, (i, j) in far_first:
        pltpu.make_async_remote_copy(
            src_ref=square_row,
            dst_ref=squares.at[slot],
            send_sem=norm_send,
            recv_sem=norm_recv,
            device_id={"section": section_at[i], "replica": peer_at[j]},
            device_id_type=MESH,
        ).start()
    pltpu.make_async_copy(rows_buf, rows_buf, row_sems.at[0, 0]).wait()
    for group in (near, far, mate, {0: cross, 1: over}):
        for copy in group.values():
            copy.wait_send()
    pltpu.make_async_copy(squares, squares, norm_recv).wait()
    pltpu.make_async_copy(squares, squares, norm_send).wait()
    norm_total = jnp.sum(part + jnp.sum(squares[...], axis=0), axis=1, keepdims=True)
    element_count = sections * row_count * width
    root_mean = jnp.sqrt(norm_total / element_count + epsilon)
    clip_factor = scale_level / root_mean
    update_ref[...] = (summed * clip_factor).astype(jnp.bfloat16)


def residual_early(early, ids_hbm, counts_hbm, gradient_hbm, residual_hbm, left_hbm, *scratch):
    grad_buf, res_buf, ids_ref, counts_ref, list_sems, load_sems, out_sems = scratch
    block_total = residual_hbm.shape[0]
    slot_count = ids_hbm.shape[1]
    step = block_total // EARLY_STEPS

    @pl.when(early())
    def _():
        lists = [
            pltpu.make_async_copy(ids_hbm, ids_ref, list_sems.at[0]),
            pltpu.make_async_copy(counts_hbm, counts_ref, list_sems.at[1]),
        ]
        for copy in lists:
            copy.start()
        loads, stores = [], []
        for c in range(EARLY_STEPS):
            part = pl.ds(c * step, step)
            loads.append(
                (
                    pltpu.make_async_copy(gradient_hbm.at[part], grad_buf.at[part], load_sems.at[0, c]),
                    pltpu.make_async_copy(residual_hbm.at[part], res_buf.at[part], load_sems.at[1, c]),
                )
            )
            stores.append(pltpu.make_async_copy(res_buf.at[part], left_hbm.at[part], out_sems.at[c]))
            for copy in loads[c]:
                copy.start()
        for copy in lists:
            copy.wait()
        for c in range(EARLY_STEPS):
            for copy in loads[c]:
                copy.wait()
            for b in range(c * step, (c + 1) * step):
                chosen = jnp.int32(0)
                for s in range(slot_count):
                    chosen = jnp.where((ids_ref[0, s] == b) & (s < counts_ref[0, 0]), 1, chosen)
                value = grad_buf[b].astype(jnp.float32) + res_buf[b]
                rounded = value.astype(jnp.bfloat16).astype(jnp.float32)
                res_buf[b] = value - jnp.where(chosen > 0, rounded, 0.0)
            stores[c].start()
        for copy in stores:
            copy.wait()


def starts_early():
    return (lax.axis_index("replica") == 0) & (lax.axis_index("section") < 2)


def deliver(replicas, early, update_ref, left_ref, early_hbm, update_hbm, left_hbm, sems):
    col_count = left_ref.shape[3]
    replica = lax.axis_index("replica")
    update_copy = pltpu.make_async_copy(update_ref, update_hbm, sems.at[replicas])
    update_copy.start()

    @pl.when(jnp.logical_not(early()))
    def _():
        copies = []
        for mask in range(replicas):
            cols = pl.ds(pl.multiple_of(flip(replica, mask) * col_count, col_count), col_count)
            copies.append(pltpu.make_async_copy(left_ref.at[mask], left_hbm.at[:, :, cols], sems.at[mask]))
        for copy in copies:
            copy.start()
        for copy in copies:
            copy.wait()

    update_copy.wait()


def per_device(sections, replicas, gradient, residual, block_ids, block_counts):
    row_count, width = gradient.shape
    block_total = row_count // BLK
    slot_count = block_ids.shape[1]
    col_count = width // replicas
    total = sections * replicas
    slot_rows = slot_count * BLK
    cap_rows = slot_count // 2 * BLK
    over_rows = slot_rows - cap_rows
    half = replicas // 2
    pair = pltpu.SemaphoreType.DMA
    gradient = gradient.reshape(block_total, BLK, width)
    residual = residual.reshape(block_total, BLK, width)
    early = pl.pallas_call(
        functools.partial(residual_early, starts_early),
        out_shape=jax.ShapeDtypeStruct(residual.shape, residual.dtype),
        in_specs=[pl.BlockSpec(memory_space=pl.ANY)] * 4,
        out_specs=pl.BlockSpec(memory_space=pltpu.HBM),
        scratch_shapes=[
            pltpu.VMEM(gradient.shape, gradient.dtype),
            pltpu.VMEM(residual.shape, residual.dtype),
            pltpu.SMEM(block_ids.shape, jnp.int32),
            pltpu.SMEM(block_counts.shape, jnp.int32),
            pair((2,)),
            pair((2, EARLY_STEPS)),
            pair((EARLY_STEPS,)),
        ],
    )(block_ids, block_counts, gradient, residual)
    update, left = pl.pallas_call(
        functools.partial(exchange, sections, replicas),
        out_shape=(
            pltpu.VMEM((row_count, col_count), jnp.bfloat16),
            pltpu.VMEM((replicas, block_total, BLK, col_count), jnp.float32),
        ),
        in_specs=[pl.BlockSpec(memory_space=pl.ANY)] * 5,
        out_specs=(pl.BlockSpec(memory_space=pltpu.VMEM),) * 2,
        scratch_shapes=[
            [pltpu.VMEM((block_total, BLK, col_count), jnp.bfloat16)] * replicas,
            [pltpu.VMEM((block_total, BLK, col_count), jnp.float32)] * replicas,
            pltpu.VMEM((replicas, slot_rows, col_count), jnp.bfloat16),
            pltpu.VMEM((1, LANES), jnp.int32),
            pltpu.SMEM(block_ids.shape, jnp.int32),
            pltpu.SMEM(block_counts.shape, jnp.int32),
            pair((2,)),
            pair((2, replicas)),
            pltpu.SemaphoreType.REGULAR,
            pltpu.VMEM((half - 1, over_rows, col_count), jnp.bfloat16),
            pltpu.VMEM((replicas - 1, 1, LANES), jnp.int32),
            pltpu.VMEM((half - 1, slot_rows, col_count), jnp.bfloat16),
            pltpu.VMEM((half, cap_rows, col_count), jnp.bfloat16),
            pltpu.VMEM((over_rows, col_count), jnp.bfloat16),
            pltpu.VMEM((over_rows, col_count), jnp.bfloat16),
            pair((2, half - 1)),
            pair((2, 1)),
            pair((2, half - 1)),
            pair((2, half)),
            pair((2, 1)),
            pltpu.VMEM((half // 2 - 1, over_rows, col_count), jnp.bfloat16),
            pltpu.VMEM((over_rows, col_count), jnp.bfloat16),
            pltpu.VMEM((over_rows, col_count), jnp.bfloat16),
            pair((2, half // 2 - 1)),
            pair((2, 1)),
            pltpu.VMEM((1, LANES), jnp.float32),
            pltpu.VMEM((total - 1, 1, LANES), jnp.float32),
            pltpu.SemaphoreType.DMA,
            pltpu.SemaphoreType.DMA,
        ],
        compiler_params=pltpu.CompilerParams(collective_id=0, has_side_effects=True),
    )(
        block_ids,
        block_counts,
        gradient,
        residual,
        early,
    )
    update, left = pl.pallas_call(
        functools.partial(deliver, replicas, starts_early),
        out_shape=(
            jax.ShapeDtypeStruct(update.shape, update.dtype),
            jax.ShapeDtypeStruct((block_total, BLK, width), left.dtype),
        ),
        in_specs=[pl.BlockSpec(memory_space=pl.ANY)] * 2 + [pl.BlockSpec(memory_space=pltpu.HBM)],
        out_specs=(pl.BlockSpec(memory_space=pltpu.HBM),) * 2,
        input_output_aliases={2: 1},
        scratch_shapes=[pltpu.SemaphoreType.DMA((replicas + 1,))],
        compiler_params=pltpu.CompilerParams(vmem_limit_bytes=1 << 20),
    )(update, left, early)
    return (left.reshape(row_count, width), update)


def solution(mesh):
    spec = P("section", "replica")
    sizes = (mesh.shape["section"], mesh.shape["replica"])
    return jax.shard_map(
        functools.partial(per_device, *sizes),
        mesh=mesh,
        in_specs=(spec,) * 4,
        out_specs=(spec, spec),
        check_vma=False,
    )
```

```python
import functools

import jax
import jax.numpy as jnp
from jax import lax
from jax.experimental import pallas as pl
from jax.experimental.pallas import tpu as pltpu
from jax.sharding import PartitionSpec as P

BLK = 8
LANES = 128
EARLY_STEPS = 2
MESH = pl.DeviceIdType.MESH

scale_level = 1.0
epsilon = 1e-06


def flip(index, mask):
    bit, out = 1, index
    while bit <= mask:
        if mask & bit:
            out = out + bit - 2 * bit * (index // bit % 2)
        bit *= 2
    return out


def exchange(
    sections,
    replicas,
    ids_hbm,
    counts_hbm,
    gradient_hbm,
    residual_hbm,
    early_hbm,
    update_ref,
    left_ref,
    grad_buf,
    res_buf,
    packed,
    target_row,
    ids_ref,
    counts_ref,
    list_sems,
    load_sems,
    ready,
    relayed,
    rows_buf,
    near_buf,
    far_buf,
    cross_buf,
    cross_in,
    relay_sems,
    row_sems,
    near_sems,
    far_sems,
    cross_sems,
    mate_buf,
    over_buf,
    near_over,
    mate_sems,
    over_sems,
    square_row,
    squares,
    norm_send,
    norm_recv,
):
    block_total, _, width = residual_hbm.shape
    row_count = block_total * BLK
    slot_count = ids_hbm.shape[1]
    slot_rows = slot_count * BLK
    cap = slot_count // 2
    cap_rows = cap * BLK
    half = replicas // 2
    col_count = width // replicas
    section = lax.axis_index("section")
    replica = lax.axis_index("replica")

    def ahead(here, extent):
        return [here] + [
            jnp.where(here + k >= extent, here + k - extent, here + k) for k in range(1, extent)
        ]

    section_at = ahead(section, sections)
    peer_at = [flip(replica, mask) for mask in range(replicas)]
    others = [(i, j) for i in range(sections) for j in range(replicas) if i + j > 0]

    lists = [
        pltpu.make_async_copy(ids_hbm, ids_ref, list_sems.at[0]),
        pltpu.make_async_copy(counts_hbm, counts_ref, list_sems.at[1]),
    ]
    for copy in lists:
        copy.start()

    quarter = replicas // 4
    part_at = replica // quarter
    lower = part_at < 2
    inner = (part_at == 1) | (part_at == 2)
    beside = [half + quarter + low for low in range(quarter)]
    beyond = [half + low for low in range(quarter)]

    def greet(i, j):
        pl.semaphore_signal(
            barrier,
            inc=1,
            device_id={"section": section_at[i], "replica": peer_at[j]},
            device_id_type=MESH,
        )

    barrier = pltpu.get_barrier_semaphore()
    for j in range(1, half):
        greet(0, j)
    for i in range(1, sections):
        greet(i, 0)
    for j in beside:
        pl.when(lower | inner)(functools.partial(greet, 0, j))
    for j in beyond:
        pl.when(lower)(functools.partial(greet, 0, j))
    greeted = half - 1 + sections - 1 + jnp.where(lower, jnp.where(inner, quarter, 0), half)

    order = list(range(replicas - 1, -1, -1))
    same = list(range(1, quarter))
    next_to = list(range(quarter, half))
    loads = {}
    for mask in order:
        cols = pl.ds(pl.multiple_of(peer_at[mask] * col_count, col_count), col_count)
        loads[mask] = (
            pltpu.make_async_copy(gradient_hbm.at[:, :, cols], grad_buf[mask], load_sems.at[0, mask]),
            pltpu.make_async_copy(residual_hbm.at[:, :, cols], res_buf[mask], load_sems.at[1, mask]),
        )
        for copy in loads[mask]:
            copy.start()

    for copy in lists:
        copy.wait()
    count = counts_ref[0, 0]
    ids = [ids_ref[0, s] for s in range(slot_count)]
    lane = lax.broadcasted_iota(jnp.int32, (1, LANES), 1)
    row = jnp.full((1, LANES), -1, jnp.int32)
    for s in range(slot_count):
        base = jnp.where(s < count, ids[s] * BLK, -2 * row_count)
        row = jnp.where(lane // BLK == s, base + lane % BLK, row)
    target_row[...] = row

    def arrive(mask):
        for copy in loads[mask]:
            copy.wait()

    def pack_slots(mask, first, last):
        for s in range(first, last, 2):
            pair = []
            for i in (s, s + 1):
                value = grad_buf[mask][ids[i]].astype(jnp.float32) + res_buf[mask][ids[i]]
                if s >= cap:
                    value = jnp.where(i < count, value, 0.0)
                pair.append(value)
            packed[mask, pl.ds(s * BLK, 2 * BLK), :] = jnp.concatenate(pair, axis=0).astype(jnp.bfloat16)

    def pack(mask):
        arrive(mask)
        pack_slots(mask, 0, slot_count)

    def make(src, dst, sems, slot, peer):
        return pltpu.make_async_remote_copy(
            src_ref=src,
            dst_ref=dst,
            send_sem=sems.at[0, slot],
            recv_sem=sems.at[1, slot],
            device_id={"replica": peer},
            device_id_type=MESH,
        )

    relay_in, near_rows, near, far_rows, far = {}, {}, {}, {}, {}
    for mask in range(1, half):
        peer = peer_at[mask]
        relay_in[mask] = make(
            packed.at[half + mask, pl.ds(cap_rows, slot_rows - cap_rows)],
            relayed.at[mask - 1],
            relay_sems,
            mask - 1,
            peer,
        )
        near_rows[mask] = make(target_row, rows_buf.at[mask - 1], row_sems, 0, peer)
        rows = pl.ds(0, slot_rows if mask in same else cap_rows)
        near[mask] = make(packed.at[mask, rows], near_buf.at[mask - 1, rows], near_sems, mask - 1, peer)
    for mask in range(half, replicas):
        peer, slot = peer_at[mask], mask - half
        far_rows[mask] = make(target_row, rows_buf.at[mask - 1], row_sems, 0, peer)
        far[mask] = make(packed.at[mask, pl.ds(0, cap_rows)], far_buf.at[slot], far_sems, slot, peer)
    mate = {}
    for mask in same:
        mate[mask] = make(
            packed.at[quarter + mask, pl.ds(cap_rows, slot_rows - cap_rows)],
            mate_buf.at[mask - 1],
            mate_sems,
            mask - 1,
            peer_at[mask],
        )
    over = make(over_buf, near_over, over_sems, 0, peer_at[quarter])
    cross = make(cross_buf, cross_in, cross_sems, 0, peer_at[half])

    def start_far(masks):
        for mask in masks:
            far_rows[mask].start()
            far[mask].start()

    def tell(mask):
        pl.semaphore_signal(ready, inc=1, device_id={"replica": peer_at[mask]}, device_id_type=MESH)

    def start_near(masks):
        for mask in masks:
            near_rows[mask].start()
            near[mask].start()

    urgent = order[: half - 1]
    for mask in urgent:
        arrive(mask)
        pack_slots(mask, cap, slot_count)
    pl.semaphore_wait(barrier, greeted)
    @pl.when(part_at == 2)
    def _():
        tell(half + quarter)
        tell(half)

    for mask in next_to[::-1] + same:
        relay_in[mask].start()
    for mask in urgent:
        pack_slots(mask, 0, cap)
    pl.when(inner)(functools.partial(start_far, beside[::-1]))
    pack(half)
    pl.when(part_at == 2)(functools.partial(start_far, beyond[::-1]))
    for mask in order[half:]:
        if mask not in urgent:
            pack(mask)
    for mask in same:
        mate[mask].start()
    @pl.when(part_at == 3)
    def _():
        start_far(beyond[::-1])
        start_far(beside[::-1])

    @pl.when(part_at == 1)
    def _():
        pl.semaphore_wait(ready, 1)
        start_far(beyond[::-1])

    for mask in range(half - 1, 0, -1):
        relay_in[mask].wait_send()

    @pl.when(part_at == 0)
    def _():
        pl.semaphore_wait(ready, 1)
        start_far(beside[::-1])
        start_far(beyond[::-1])

    start_near(next_to[::-1] + same)

    for b in range(block_total):
        chosen = jnp.int32(0)
        for s in range(slot_count):
            chosen = jnp.where((ids[s] == b) & (s < count), 1, chosen)
        for mask in order:
            value = grad_buf[mask][b].astype(jnp.float32) + res_buf[mask][b]
            rounded = value.astype(jnp.bfloat16).astype(jnp.float32)
            left_ref[mask, b] = value - jnp.where(chosen > 0, rounded, 0.0)

    def place(wanted, block):
        row_iota = lax.broadcasted_iota(jnp.int32, (row_count, wanted.shape[1]), 0)
        hot = jnp.where(row_iota == wanted, 1.0, 0.0).astype(jnp.bfloat16)
        return jnp.dot(hot, block, preferred_element_type=jnp.float32)

    crossing = packed[half, cap_rows:, :].astype(jnp.float32)
    for mask in range(half - 1, 0, -1):
        relay_in[mask].wait_recv()
        crossing = crossing + relayed[mask - 1].astype(jnp.float32)
    cross_buf[...] = crossing.astype(jnp.bfloat16)
    cross.start()
    beside_over = packed[quarter, cap_rows:, :].astype(jnp.float32)
    for mask in same:
        mate[mask].wait_recv()
        beside_over = beside_over + mate_buf[mask - 1].astype(jnp.float32)
    over_buf[...] = beside_over.astype(jnp.bfloat16)
    over.start()

    summed = place(target_row[:, :slot_rows], packed[0])
    pltpu.make_async_copy(rows_buf, rows_buf, row_sems.at[1, 0]).wait()
    wanted = jnp.full((1, slot_rows), -1, jnp.int32)
    for mask in range(half - 1, 0, -1):
        near[mask].wait_recv()
        theirs = rows_buf[mask - 1][:, :slot_rows]
        if mask in same:
            summed = summed + place(theirs, near_buf[mask - 1])
        else:
            wanted = jnp.maximum(wanted, theirs)
            summed = summed + place(theirs[:, :cap_rows], near_buf[mask - 1, :cap_rows])
    far_wanted = jnp.full((1, slot_rows), -1, jnp.int32)
    for mask in range(replicas - 1, half - 1, -1):
        far[mask].wait_recv()
        theirs = rows_buf[mask - 1][:, :slot_rows]
        far_wanted = jnp.maximum(far_wanted, theirs)
        summed = summed + place(theirs[:, :cap_rows], far_buf[mask - half])
    over.wait_recv()
    summed = summed + place(wanted[:, cap_rows:], near_over[...])
    cross.wait_recv()
    summed = summed + place(far_wanted[:, cap_rows:], cross_in[...])

    lanes = jnp.sum(summed * summed, axis=0, keepdims=True)
    part = lanes[:, :LANES]
    for j in range(1, col_count // LANES):
        part = part + lanes[:, j * LANES : (j + 1) * LANES]
    square_row[...] = part

    far_first = sorted(
        enumerate(others),
        key=lambda entry: (entry[1][0] * 2 // sections, entry[1][0] % 2 == 0, entry[1][1]),
        reverse=True,
    )
    for slot, (i, j) in far_first:
        pltpu.make_async_remote_copy(
            src_ref=square_row,
            dst_ref=squares.at[slot],
            send_sem=norm_send,
            recv_sem=norm_recv,
            device_id={"section": section_at[i], "replica": peer_at[j]},
            device_id_type=MESH,
        ).start()
    pltpu.make_async_copy(rows_buf, rows_buf, row_sems.at[0, 0]).wait()
    for group in (near, far, mate, {0: cross, 1: over}):
        for copy in group.values():
            copy.wait_send()
    pltpu.make_async_copy(squares, squares, norm_recv).wait()
    pltpu.make_async_copy(squares, squares, norm_send).wait()
    norm_total = jnp.sum(part + jnp.sum(squares[...], axis=0), axis=1, keepdims=True)
    element_count = sections * row_count * width
    root_mean = jnp.sqrt(norm_total / element_count + epsilon)
    clip_factor = scale_level / root_mean
    update_ref[...] = (summed * clip_factor).astype(jnp.bfloat16)


def residual_early(early, ids_hbm, counts_hbm, gradient_hbm, residual_hbm, left_hbm, *scratch):
    grad_buf, res_buf, ids_ref, counts_ref, list_sems, load_sems, out_sems = scratch
    block_total = residual_hbm.shape[0]
    slot_count = ids_hbm.shape[1]
    step = block_total // EARLY_STEPS

    @pl.when(early())
    def _():
        lists = [
            pltpu.make_async_copy(ids_hbm, ids_ref, list_sems.at[0]),
            pltpu.make_async_copy(counts_hbm, counts_ref, list_sems.at[1]),
        ]
        for copy in lists:
            copy.start()
        loads, stores = [], []
        for c in range(EARLY_STEPS):
            part = pl.ds(c * step, step)
            loads.append(
                (
                    pltpu.make_async_copy(gradient_hbm.at[part], grad_buf.at[part], load_sems.at[0, c]),
                    pltpu.make_async_copy(residual_hbm.at[part], res_buf.at[part], load_sems.at[1, c]),
                )
            )
            stores.append(pltpu.make_async_copy(res_buf.at[part], left_hbm.at[part], out_sems.at[c]))
            for copy in loads[c]:
                copy.start()
        for copy in lists:
            copy.wait()
        for c in range(EARLY_STEPS):
            for copy in loads[c]:
                copy.wait()
            for b in range(c * step, (c + 1) * step):
                chosen = jnp.int32(0)
                for s in range(slot_count):
                    chosen = jnp.where((ids_ref[0, s] == b) & (s < counts_ref[0, 0]), 1, chosen)
                value = grad_buf[b].astype(jnp.float32) + res_buf[b]
                rounded = value.astype(jnp.bfloat16).astype(jnp.float32)
                res_buf[b] = value - jnp.where(chosen > 0, rounded, 0.0)
            stores[c].start()
        for copy in stores:
            copy.wait()


def starts_early():
    return (lax.axis_index("replica") == 0) & (lax.axis_index("section") < 2)


def deliver(replicas, early, update_ref, left_ref, early_hbm, update_hbm, left_hbm, sems):
    col_count = left_ref.shape[3]
    replica = lax.axis_index("replica")
    update_copy = pltpu.make_async_copy(update_ref, update_hbm, sems.at[replicas])
    update_copy.start()

    @pl.when(jnp.logical_not(early()))
    def _():
        copies = []
        for mask in range(replicas):
            cols = pl.ds(pl.multiple_of(flip(replica, mask) * col_count, col_count), col_count)
            copies.append(pltpu.make_async_copy(left_ref.at[mask], left_hbm.at[:, :, cols], sems.at[mask]))
        for copy in copies:
            copy.start()
        for copy in copies:
            copy.wait()

    update_copy.wait()


def per_device(sections, replicas, gradient, residual, block_ids, block_counts):
    row_count, width = gradient.shape
    block_total = row_count // BLK
    slot_count = block_ids.shape[1]
    col_count = width // replicas
    total = sections * replicas
    slot_rows = slot_count * BLK
    cap_rows = slot_count // 2 * BLK
    over_rows = slot_rows - cap_rows
    half = replicas // 2
    pair = pltpu.SemaphoreType.DMA
    gradient = gradient.reshape(block_total, BLK, width)
    residual = residual.reshape(block_total, BLK, width)
    early = pl.pallas_call(
        functools.partial(residual_early, starts_early),
        out_shape=jax.ShapeDtypeStruct(residual.shape, residual.dtype),
        in_specs=[pl.BlockSpec(memory_space=pl.ANY)] * 4,
        out_specs=pl.BlockSpec(memory_space=pltpu.HBM),
        scratch_shapes=[
            pltpu.VMEM(gradient.shape, gradient.dtype),
            pltpu.VMEM(residual.shape, residual.dtype),
            pltpu.SMEM(block_ids.shape, jnp.int32),
            pltpu.SMEM(block_counts.shape, jnp.int32),
            pair((2,)),
            pair((2, EARLY_STEPS)),
            pair((EARLY_STEPS,)),
        ],
    )(block_ids, block_counts, gradient, residual)
    update, left = pl.pallas_call(
        functools.partial(exchange, sections, replicas),
        out_shape=(
            pltpu.VMEM((row_count, col_count), jnp.bfloat16),
            pltpu.VMEM((replicas, block_total, BLK, col_count), jnp.float32),
        ),
        in_specs=[pl.BlockSpec(memory_space=pl.ANY)] * 5,
        out_specs=(pl.BlockSpec(memory_space=pltpu.VMEM),) * 2,
        scratch_shapes=[
            [pltpu.VMEM((block_total, BLK, col_count), jnp.bfloat16)] * replicas,
            [pltpu.VMEM((block_total, BLK, col_count), jnp.float32)] * replicas,
            pltpu.VMEM((replicas, slot_rows, col_count), jnp.bfloat16),
            pltpu.VMEM((1, LANES), jnp.int32),
            pltpu.SMEM(block_ids.shape, jnp.int32),
            pltpu.SMEM(block_counts.shape, jnp.int32),
            pair((2,)),
            pair((2, replicas)),
            pltpu.SemaphoreType.REGULAR,
            pltpu.VMEM((half - 1, over_rows, col_count), jnp.bfloat16),
            pltpu.VMEM((replicas - 1, 1, LANES), jnp.int32),
            pltpu.VMEM((half - 1, slot_rows, col_count), jnp.bfloat16),
            pltpu.VMEM((half, cap_rows, col_count), jnp.bfloat16),
            pltpu.VMEM((over_rows, col_count), jnp.bfloat16),
            pltpu.VMEM((over_rows, col_count), jnp.bfloat16),
            pair((2, half - 1)),
            pair((2, 1)),
            pair((2, half - 1)),
            pair((2, half)),
            pair((2, 1)),
            pltpu.VMEM((half // 2 - 1, over_rows, col_count), jnp.bfloat16),
            pltpu.VMEM((over_rows, col_count), jnp.bfloat16),
            pltpu.VMEM((over_rows, col_count), jnp.bfloat16),
            pair((2, half // 2 - 1)),
            pair((2, 1)),
            pltpu.VMEM((1, LANES), jnp.float32),
            pltpu.VMEM((total - 1, 1, LANES), jnp.float32),
            pltpu.SemaphoreType.DMA,
            pltpu.SemaphoreType.DMA,
        ],
        compiler_params=pltpu.CompilerParams(collective_id=0, has_side_effects=True),
    )(
        block_ids,
        block_counts,
        gradient,
        residual,
        early,
    )
    update, left = pl.pallas_call(
        functools.partial(deliver, replicas, starts_early),
        out_shape=(
            jax.ShapeDtypeStruct(update.shape, update.dtype),
            jax.ShapeDtypeStruct((block_total, BLK, width), left.dtype),
        ),
        in_specs=[pl.BlockSpec(memory_space=pl.ANY)] * 2 + [pl.BlockSpec(memory_space=pltpu.HBM)],
        out_specs=(pl.BlockSpec(memory_space=pltpu.HBM),) * 2,
        input_output_aliases={2: 1},
        scratch_shapes=[pltpu.SemaphoreType.DMA((replicas + 1,))],
        compiler_params=pltpu.CompilerParams(vmem_limit_bytes=1 << 20),
    )(update, left, early)
    return (left.reshape(row_count, width), update)


def solution(mesh):
    spec = P("section", "replica")
    sizes = (mesh.shape["section"], mesh.shape["replica"])
    return jax.shard_map(
        functools.partial(per_device, *sizes),
        mesh=mesh,
        in_specs=(spec,) * 4,
        out_specs=(spec, spec),
        check_vma=False,
    )
```
